16 devices in a mesh: dp: 2 (over y, z), sp: 8 (over x, core).
Axes of the slice: x: 4, y: 2, z: 1, core: 2. Of those that a mesh axis runs over, the one named last changes fastest.
The devices are a block of a 4x4x8 slice.
Arguments:
- x: bfloat16 [8192, 3840], P(('dp', 'sp')), parts along dimension 0
- gain: bfloat16 [3840], replicated
- wq: bfloat16 [3840, 4096], replicated
- wk: bfloat16 [3840, 2048], replicated
- wv: bfloat16 [3840, 2048], replicated
- wo: bfloat16 [4096, 3840], replicated
Outputs:
- output: bfloat16 [8192, 3840], P(('dp', 'sp')), parts along dimension 0
There are 2 independent parts. The reference program is written for one: setup_inputs(seed, part) draws one part's arguments, and reference() takes and returns one part's arrays. A program takes and returns all parts, laid end to end along the dimension named above; an argument that names none is the same for every part.
All inputs are finite; a program needn't handle non-finite values.
Results may differ from the reference program's by a relative error of at most 0.012.
Values are sent between devices in bfloat16 or wider.
A program may use at most 768 MiB of HBM per device.

```python
import jax
import jax.numpy as jnp
from jax import lax

ROWS = 4096
D = 3840
HEADS = 16
KV_HEADS = 8
HEAD = 256
THETA = 10000


def setup_inputs(seed: int = 0, part: int = 0) -> dict:
    kx, kn, kq, kk, kv, ko = jax.random.split(jax.random.key(seed), 6)

    def weights(key, rows, columns):
        return jax.random.normal(key, (rows, columns), jnp.float32) * rows**-0.5

    drawn = {
        "x": jax.random.normal(jax.random.fold_in(kx, part), (ROWS, D), jnp.float32),
        "gain": 1 + 0.1 * jax.random.normal(kn, (D,), jnp.float32),
        "wq": 2 * weights(kq, D, HEADS * HEAD),
        "wk": 2 * weights(kk, D, KV_HEADS * HEAD),
        "wv": 4 * weights(kv, D, KV_HEADS * HEAD),
        "wo": weights(ko, HEADS * HEAD, D),
    }
    return {k: v.astype(jnp.bfloat16) for k, v in drawn.items()}


def normed(x, gain):
    wide = x.astype(jnp.float32)
    scale = lax.rsqrt(jnp.mean(wide * wide, -1, keepdims=True) + 1e-6)
    return (wide * scale * gain.astype(jnp.float32)).astype(jnp.bfloat16)


def turned(t, place, theta):
    half = t.shape[-1] // 2
    angle = place.astype(jnp.float32)[:, None] * theta ** (-jnp.arange(half, dtype=jnp.float32) / half)
    cos, sin = jnp.cos(angle)[:, None], jnp.sin(angle)[:, None]
    a, b = t[..., :half].astype(jnp.float32), t[..., half:].astype(jnp.float32)
    return jnp.concatenate([a * cos - b * sin, b * cos + a * sin], -1).astype(jnp.bfloat16)


def matmul(a, w):
    return jnp.dot(a, w, preferred_element_type=jnp.float32).astype(jnp.bfloat16)


def einsum(form, a, b):
    return jnp.einsum(form, a.astype(jnp.float32), b.astype(jnp.float32))


def attention(q, k, v):
    scores = einsum("tgsd,ugd->gstu", q, k) * q.shape[-1] ** -0.5
    token = jnp.arange(q.shape[0])
    scores = jnp.where(token[:, None] >= token, scores, -jnp.inf)
    weights = jax.nn.softmax(scores, -1).astype(jnp.bfloat16)
    return einsum("gstu,ugd->tgsd", weights, v).astype(jnp.bfloat16)


def reference(x, gain, wq, wk, wv, wo):
    a, place = normed(x, gain), jnp.arange(ROWS)
    q = turned(matmul(a, wq).reshape(ROWS, HEADS, HEAD), place, THETA).reshape(ROWS, KV_HEADS, -1, HEAD)
    k = turned(matmul(a, wk).reshape(ROWS, KV_HEADS, HEAD), place, THETA)
    v = matmul(a, wv).reshape(ROWS, KV_HEADS, HEAD)
    seen = attention(q, k, v).reshape(ROWS, HEADS * HEAD)
    return (x.astype(jnp.float32) + jnp.dot(seen, wo, preferred_element_type=jnp.float32)).astype(jnp.bfloat16)
```

```python
import functools

import jax
import jax.numpy as jnp
from jax import lax
from jax.experimental import pallas as pl
from jax.experimental.pallas import tpu as pltpu
from jax.sharding import PartitionSpec as P

HEAD = 256
THETA = 10000
NEG = -1e30
HIDDEN = 2 * NEG
LOG2E = 1.4426950408889634
MESH = pl.DeviceIdType.MESH
SLOTS = 4
AWAY = 3
Q_ORDER = (3, 0, 1, 2)
NONE, FULL, DIAG = 0, 1, 2

PLACE = {
    0: {(1, 3): 4, (2, 3): 5, (3, 3): 6, (1, 0): 7},
    1: {(0, 0): 4, (0, 1): 5, (0, 2): 6, (0, 3): 7, (2, 3): 8},
    2: {(0, s): 4 + s for s in range(4)} | {(1, s): 8 + s for s in range(4)},
    3: {(j, s): 4 + 3 * j + s for j in range(3) for s in range(3)},
}
for _p in PLACE:
    PLACE[_p] |= {(_p, s): s for s in range(SLOTS)}
N_KV = 13

AFTER_KV = {
    (0, 0): [(1, 0, 0), (3, 0, 0)],
    (0, 1): [(1, 0, 1), (3, 0, 1)],
    (0, 2): [(1, 0, 2), (3, 0, 2)],
    (0, 3): [(1, 0, 3)],
    (1, 0): [(2, 1, 0), (0, 1, 0)],
    (1, 1): [(2, 1, 1)],
    (1, 2): [(2, 1, 2)],
    (1, 3): [(2, 1, 3), (0, 1, 3)],
    (2, 0): [(3, 2, 0)],
    (2, 1): [(3, 2, 1)],
    (2, 2): [(3, 2, 2)],
    (2, 3): [(1, 2, 3)],
    (3, 3): [(0, 3, 3)],
}
PASS_Q = {(3, 1): [(2, 0, 0)]}
PASS_T = {
    (0, 1): [(3, 1, 0)],
    (1, 2): [(0, 2, 3)],
    (1, 7): [(2, 0, 3)],
    (2, 6): [(3, 1, 1)],
    (2, 8): [(3, 1, 2)],
    (3, 5): [(2, 0, 1)],
    (3, 7): [(2, 0, 2)],
}
TASKS = {
    0: [(DIAG, 0, 0, 0, 1), (DIAG, 1, 0, 1, 1), (DIAG, 2, 0, 2, 1), (DIAG, 3, 0, 3, 1), (FULL, 4, 1, 3, 0), (FULL, 4, 0, 3, 0),
        (DIAG, 4, 3, 3, 0), (FULL, 4, 2, 3, 1)],
    1: [(DIAG, s, 1, s, 0) for s in range(4)] + [(FULL, s, 0, s, 1) for s in range(4)],
    2: [(DIAG, s, 2, s, 0) for s in range(4)] + [(FULL, 0, 1, 0, 0), (FULL, 0, 0, 0, 1), (FULL, 1, 1, 1, 0), (FULL, 1, 0, 1, 1),
        (FULL, 2, 1, 2, 0), (FULL, 2, 0, 2, 1), (FULL, 3, 1, 3, 0), (FULL, 3, 0, 3, 1)],
    3: [(DIAG, s, 3, s, 0) for s in range(3)] + [(FULL, 0, 0, 0, 0), (FULL, 0, 2, 0, 0), (FULL, 1, 0, 1, 0), (FULL, 1, 2, 1, 0),
        (FULL, 2, 0, 2, 0), (FULL, 2, 2, 2, 0), (FULL, 0, 1, 0, 1), (FULL, 1, 1, 1, 1), (FULL, 2, 1, 2, 1)],
}
N_TASKS = max(len(t) for t in TASKS.values())
Q_WAIT = 4

SENDS = {p: [] for p in range(4)}
for _table in (AFTER_KV, PASS_Q, PASS_T):
    for (_p, _), _list in _table.items():
        SENDS[_p] += _list
N_SENDS = max(len(v) for v in SENDS.values())


def _waits(p):
    passed = {m[1:] for table in (PASS_Q, PASS_T) for (chip, _), messages in table.items() if chip == p for m in messages}
    waits = {}
    for n, (_, _, j, s, _) in enumerate(TASKS[p]):
        if j != p and (j, s) not in passed:
            waits[n] = (j, s)
    return waits


def _pick(chip, step, table, default):
    out = jnp.int32(default)
    for p, row in table.items():
        for n, v in enumerate(row):
            if v != default:
                out = jnp.where((chip == p) & (step == n), jnp.int32(v), out)
    return out


def _dot(a, b, ca, cb):
    return lax.dot_general(a, b, (((ca,), (cb,)), ((), ())), preferred_element_type=jnp.float32)


def _kernel(x_ref, gain_ref, cos_ref, sin_ref, wq_ref, wk_ref, wv_ref, o_ref, a, w, q, kv, mix, top, ofin, osend,
            w_sem, x_sem, out_sem, a_sem, kv_send, kv_recv, q_sem, o_send, o_recv):
    own, depth = x_ref.shape
    tokens = 2 * own
    me = lax.axis_index("sp")
    chip, core = lax.div(me, 2), lax.rem(me, 2)
    other = 2 * chip + 1 - core
    e = HEAD**-0.5 * LOG2E
    group = 8

    def half(h):
        return pl.ds(pl.multiple_of(h * own, own), own)

    def columns(n, width):
        return pl.ds(pl.multiple_of(n * width, width), width)

    def weights(step):
        at = lax.rem(step, 2)
        n = core * SLOTS + step
        return (pltpu.make_async_copy(wk_ref.at[:, columns(n, HEAD)], w.at[at, :, pl.ds(0, HEAD)], w_sem.at[at]),
                pltpu.make_async_copy(wv_ref.at[:, columns(n, HEAD)], w.at[at, :, pl.ds(HEAD, HEAD)], w_sem.at[at]))

    def query_slot(i):
        return lax.rem(i + 3, SLOTS)

    def query_weights(i):
        at = lax.rem(i, 2)
        n = core * SLOTS + query_slot(i)
        return pltpu.make_async_copy(wq_ref.at[:, columns(n, 2 * HEAD)], w.at[at], w_sem.at[at])

    load_x = pltpu.make_async_copy(x_ref, a.at[half(core)], x_sem)
    load_x.start()
    for copy in weights(0) + weights(1):
        copy.start()

    barrier = pltpu.get_barrier_semaphore()
    for n in range(1, group):
        pl.semaphore_signal(barrier, inc=1, device_id={"sp": lax.rem(me + n, group)}, device_id_type=MESH)

    def send(p, m):
        to, j, s = m
        n = SENDS[p].index(m)
        return pltpu.make_async_remote_copy(
            src_ref=kv.at[PLACE[p][j, s]], dst_ref=kv.at[PLACE[to][j, s]], send_sem=kv_send.at[n],
            recv_sem=kv_recv.at[PLACE[to][j, s] - SLOTS], device_id={"sp": 2 * to + core}, device_id_type=MESH)

    def arrived(p, j, s):
        at = PLACE[p][j, s]
        pltpu.make_async_remote_copy(
            src_ref=kv.at[at], dst_ref=kv.at[at], send_sem=kv_send.at[0], recv_sem=kv_recv.at[at - SLOTS],
            device_id={"sp": other}, device_id_type=MESH).wait_recv()

    def act(table, step, relay):
        for p in range(4):
            steps = [(n, messages) for (c, n), messages in table.items() if c == p]
            if steps:
                @pl.when(chip == p)
                def _(p=p, steps=steps):
                    for n, messages in steps:
                        @pl.when(step == n)
                        def _(p=p, messages=messages):
                            for m in messages:
                                if relay:
                                    arrived(p, *m[1:])
                                send(p, m).start()

    send_a = pltpu.make_async_remote_copy(
        src_ref=a.at[half(core)], dst_ref=a.at[half(core)], send_sem=a_sem.at[0], recv_sem=a_sem.at[1],
        device_id={"sp": other}, device_id_type=MESH)
    recv_a = pltpu.make_async_remote_copy(
        src_ref=a.at[half(1 - core)], dst_ref=a.at[half(1 - core)], send_sem=a_sem.at[0], recv_sem=a_sem.at[1],
        device_id={"sp": other}, device_id_type=MESH)
    send_q = pltpu.make_async_remote_copy(
        src_ref=q.at[AWAY], dst_ref=q.at[SLOTS], send_sem=q_sem.at[0], recv_sem=q_sem.at[1],
        device_id={"sp": core}, device_id_type=MESH)

    def send_o(source, head, to):
        return pltpu.make_async_remote_copy(
            src_ref=osend.at[source], dst_ref=ofin.at[:, columns(head, 2 * HEAD)], send_sem=o_send.at[source],
            recv_sem=o_recv.at[head], device_id={"sp": to}, device_id_type=MESH)

    top[...] = jnp.full(top.shape, NEG, jnp.float32)
    mix[...] = jnp.zeros(mix.shape, jnp.float32)
    load_x.wait()
    rows = 16

    def norm(i, _):
        here = pl.ds(pl.multiple_of(core * own + i * rows, rows), rows)
        wide = a[here, :].astype(jnp.float32)
        scale = lax.rsqrt(jnp.mean(wide * wide, -1, keepdims=True) + 1e-6)
        a[here, :] = (wide * scale * gain_ref[...]).astype(a.dtype)

    lax.fori_loop(0, own // rows, norm, None)
    pl.semaphore_wait(barrier, group - 1)
    send_a.start()

    def turned(t, cos, sin):
        t = t.astype(jnp.bfloat16).astype(jnp.float32)
        u, v = t[:, : HEAD // 2], t[:, HEAD // 2 :]
        return jnp.concatenate([u * cos - v * sin, v * cos + u * sin], -1).astype(jnp.bfloat16)

    def kv_step(s, _):
        at = lax.rem(s, 2)
        for copy in weights(s):
            copy.wait()

        def part(i, _):
            h = lax.rem(core + i, 2)

            @pl.when((s == 0) & (i == 1))
            def _():
                recv_a.wait_recv()

            got = jnp.dot(a[half(h), :], w[at], preferred_element_type=jnp.float32)
            kv[s, half(h), :] = turned(got[:, :HEAD], cos_ref[half(h), :], sin_ref[half(h), :])
            values = got[:, HEAD:].astype(jnp.bfloat16).T
            for b in range(own // HEAD):
                place = pl.ds(pl.multiple_of(tokens + h * own + b * HEAD, HEAD), HEAD)
                kv[s, place, :] = values[:, b * HEAD : (b + 1) * HEAD]

        lax.fori_loop(0, 2, part, None)

        @pl.when(s < SLOTS - 2)
        def _():
            for copy in weights(s + 2):
                copy.start()

        @pl.when(s >= SLOTS - 2)
        def _():
            query_weights(s - (SLOTS - 2)).start()

        act(AFTER_KV, s, False)

    lax.fori_loop(0, SLOTS, kv_step, None)

    def q_step(i, _):
        at = lax.rem(i, 2)
        s = query_slot(i)
        query_weights(i).wait()

        def part(h, _):
            got = jnp.dot(a[half(h), :], w[at], preferred_element_type=jnp.float32)
            for g in range(2):
                place = pl.ds(pl.multiple_of(g * tokens + h * own, own), own)
                q[s, place, :] = turned(got[:, g * HEAD : (g + 1) * HEAD], cos_ref[half(h), :], sin_ref[half(h), :])

        lax.fori_loop(0, 2, part, None)

        @pl.when(i < SLOTS - 2)
        def _():
            query_weights(i + 2).start()

        @pl.when((i == 0) & (chip == 3))
        def _():
            send_q.start()

        act(PASS_Q, i, True)

    lax.fori_loop(0, SLOTS, q_step, None)

    strip = own
    n_strips = 2 * tokens // strip
    ones = jnp.ones((8, strip), jnp.bfloat16)

    def block(qs, at, j, strips):
        keys = kv[at, pl.ds(pl.multiple_of(j * strip, strip), strip), :]
        values = [kv[at, pl.ds(pl.multiple_of(tokens + j * strip + b * HEAD, HEAD), HEAD), :] for b in range(strip // HEAD)]
        values = jnp.concatenate([jnp.concatenate(values, axis=1), ones], axis=0)
        spans = [pl.ds(n * strip, strip) for n, _ in strips]
        scores = [_dot(keys, q[qs, span, :], 1, 1) for span in spans]
        weights, keeps = [], []
        for (_, masked), span, s in zip(strips, spans, scores):
            if masked:
                seen = lax.broadcasted_iota(jnp.int32, s.shape, 1) >= lax.broadcasted_iota(jnp.int32, s.shape, 0)
                s = jnp.where(seen, s, HIDDEN)
            old = top[qs, :, span]
            new = jnp.maximum(old, s.max(axis=0, keepdims=True))
            top[qs, :, span] = new
            weights.append(jnp.exp2((s - new) * e).astype(jnp.bfloat16))
            keeps.append(jnp.exp2((old - new) * e))
        for span, p, keep in zip(spans, weights, keeps):
            mix[qs, :, span] = mix[qs, :, span] * keep + _dot(values, p, 1, 0)

    kind_of = {p: [t[0] for t in ts] for p, ts in TASKS.items()}
    slot_of = {p: [t[1] for t in ts] for p, ts in TASKS.items()}
    place_of = {p: [PLACE[p][t[2], t[3]] for t in ts] for p, ts in TASKS.items()}
    ends = {p: [t[4] for t in ts] for p, ts in TASKS.items()}

    def task(n, _):
        act(PASS_T, n, True)
        for p in range(4):
            @pl.when(chip == p)
            def _(p=p):
                for t, (j, s) in _waits(p).items():
                    @pl.when(n == t)
                    def _(p=p, j=j, s=s):
                        arrived(p, j, s)

        @pl.when((chip == 0) & (n == Q_WAIT))
        def _():
            send_q.wait_recv()

        kind, qs = _pick(chip, n, kind_of, 0), _pick(chip, n, slot_of, 0)
        at, end = _pick(chip, n, place_of, 0), _pick(chip, n, ends, 0)

        @pl.when(kind == FULL)
        def _():
            lax.fori_loop(0, tokens // strip, lambda j, _: block(qs, at, j, [(i, False) for i in range(n_strips)]), None)

        @pl.when(kind == DIAG)
        def _():
            block(qs, at, 0, [(0, True), (1, False), (2, True), (3, False)])
            block(qs, at, 1, [(1, True), (3, True)])

        @pl.when(end == 1)
        def _():
            def finish(h, _):
                local = (h == core) & (qs < SLOTS)
                source = jnp.where(qs < SLOTS, qs, SLOTS + h)
                for g in range(2):
                    span = pl.ds(pl.multiple_of(g * tokens + h * own, own), own)
                    out = (mix[qs, :HEAD, span] * (1 / mix[qs, HEAD : HEAD + 1, span])).T.astype(jnp.bfloat16)

                    @pl.when(local)
                    def _():
                        ofin[:, pl.ds(pl.multiple_of((core * SLOTS + qs) * 2 * HEAD + g * HEAD, HEAD), HEAD)] = out

                    @pl.when(jnp.logical_not(local))
                    def _():
                        osend[source, :, g * HEAD : (g + 1) * HEAD] = out

            lax.fori_loop(0, 2, finish, None)
            head = core * SLOTS

            @pl.when(qs < SLOTS)
            def _():
                send_o(qs, head + qs, other).start()

            @pl.when(qs == SLOTS)
            def _():
                for h in range(2):
                    send_o(SLOTS + h, head + AWAY, 6 + h).start()

    lax.fori_loop(0, N_TASKS, task, None)

    def o_arrived(head):
        pltpu.make_async_remote_copy(
            src_ref=osend.at[0], dst_ref=ofin.at[:, columns(head, 2 * HEAD)], send_sem=o_send.at[0],
            recv_sem=o_recv.at[head], device_id={"sp": other}, device_id_type=MESH).wait_recv()

    for s in range(SLOTS):
        o_arrived((1 - core) * SLOTS + s)

    @pl.when(chip == 3)
    def _():
        o_arrived(core * SLOTS + AWAY)

    put = pltpu.make_async_copy(ofin, o_ref, out_sem)
    put.start()
    send_a.wait_send()
    for p in range(4):
        @pl.when(chip == p)
        def _(p=p):
            for m in SENDS[p]:
                send(p, m).wait_send()
    for s in range(SLOTS - 1):
        send_o(s, core * SLOTS + s, other).wait_send()

    @pl.when(chip != 3)
    def _():
        send_o(AWAY, core * SLOTS + AWAY, other).wait_send()

    @pl.when(chip == 3)
    def _():
        send_q.wait_send()

    @pl.when(chip == 0)
    def _():
        for h in range(2):
            send_o(SLOTS + h, core * SLOTS + AWAY, 6 + h).wait_send()

    put.wait()


def attended(x, gain, wq, wk, wv, cos, sin):
    own, depth = x.shape
    tokens = 2 * own
    low = jnp.bfloat16
    anywhere, vmem = pl.BlockSpec(memory_space=pl.ANY), pl.BlockSpec(memory_space=pltpu.VMEM)
    dma = pltpu.SemaphoreType.DMA
    return pl.pallas_call(
        _kernel,
        out_shape=jax.ShapeDtypeStruct((own, wq.shape[1]), low),
        in_specs=[anywhere, vmem, vmem, vmem, anywhere, anywhere, anywhere],
        out_specs=anywhere,
        scratch_shapes=[
            pltpu.VMEM((tokens, depth), low),
            pltpu.VMEM((2, depth, 2 * HEAD), low),
            pltpu.VMEM((SLOTS + 1, 2 * tokens, HEAD), low),
            pltpu.VMEM((N_KV, 2 * tokens, HEAD), low),
            pltpu.VMEM((SLOTS + 1, HEAD + 8, 2 * tokens), jnp.float32),
            pltpu.VMEM((SLOTS + 1, 1, 2 * tokens), jnp.float32),
            pltpu.VMEM((own, wq.shape[1]), low),
            pltpu.VMEM((SLOTS + 2, own, 2 * HEAD), low),
            dma((2,)), dma(()), dma(()), dma((2,)), dma((N_SENDS,)), dma((N_KV - SLOTS,)), dma((2,)), dma((SLOTS + 2,)), dma((2 * SLOTS,)),
        ],
        compiler_params=pltpu.CompilerParams(collective_id=0, has_side_effects=True, vmem_limit_bytes=67043328),
        cost_estimate=pl.CostEstimate(flops=50 * 10**9, bytes_accessed=40 * 10**6, transcendentals=20 * 10**6),
    )(x, gain.astype(jnp.float32)[None], cos, sin, wq, wk, wv)


def solution(mesh):
    def step(x, gain, wq, wk, wv, wo):
        own = x.shape[0]
        me = lax.axis_index("sp")
        place = (me // 2) * 2 * own + jnp.arange(2 * own)
        angle = place.astype(jnp.float32)[:, None] * THETA ** (-jnp.arange(HEAD // 2, dtype=jnp.float32) / (HEAD // 2))
        seen = attended(x, gain, wq, wk, wv, jnp.cos(angle), jnp.sin(angle))
        y = jnp.dot(seen, wo, preferred_element_type=jnp.float32)
        return (x.astype(jnp.float32) + y).astype(jnp.bfloat16)

    tokens, whole = P(("dp", "sp"), None), P(None, None)
    return jax.shard_map(
        step,
        mesh=mesh,
        in_specs=(tokens, P(None), whole, whole, whole, whole),
        out_specs=tokens,
        check_vma=False,
    )
```

```python
import functools

import jax
import jax.numpy as jnp
import numpy as np
from jax import lax
from jax.experimental import pallas as pl
from jax.experimental.pallas import tpu as pltpu
from jax.sharding import PartitionSpec as P

HEAD = 256
THETA = 10000
NEG = -1e30
HIDDEN = 2 * NEG
LOG2E = 1.4426950408889634
MESH = pl.DeviceIdType.MESH
SLOTS = 4
AWAY = 3
NONE, FULL, DIAG, PROJECT = 0, 1, 2, 3

PLACE = {
    0: {(1, 3): 4, (2, 3): 5, (3, 3): 6, (1, 0): 7},
    1: {(0, 0): 4, (0, 1): 5, (0, 2): 6, (0, 3): 7, (2, 3): 8},
    2: {(0, s): 4 + s for s in range(4)} | {(1, s): 8 + s for s in range(4)},
    3: {(j, s): 4 + 3 * j + s for j in range(3) for s in range(3)},
}
for _p in PLACE:
    PLACE[_p] |= {(_p, s): s for s in range(SLOTS)}
N_KV = 13

AFTER_KV = {(0, 0): (1, 3), (0, 1): (1, 3), (0, 2): (1, 3), (0, 3): (1,), (1, 0): (2, 0), (1, 1): (2,), (1, 2): (2,), (1, 3): (2, 0),
            (2, 0): (3,), (2, 1): (3,), (2, 2): (3,), (2, 3): (1,), (3, 3): (0,)}
PASS_Q = {(3, 0): [(2, 0, 0, 0)], (3, 1): [(2, 0, 1, 0)], (3, 3): [(2, 0, 0, 1)]}
PASS_T = {
    (0, 1): [(3, 1, 0, 0), (3, 1, 0, 1)],
    (1, 2): [(0, 2, 3, 0), (0, 2, 3, 1)],
    (3, 2): [(2, 0, 1, 1)],
    (3, 6): [(2, 0, 2, 0)],
}
PASS_IN = {0: {}, 1: {(0, 3): 2}, 2: {(1, 1): 3, (1, 2): 3}, 3: {(0, 2): 2}}


def _diag(p, slots):
    return [(DIAG, s, p, s, 0) for s in slots]


TASKS = {
    0: [(DIAG, s, 0, s, 1) for s in range(4)] + [(PROJECT, 0, 0, 0, 0), (PROJECT, 1, 0, 0, 0), (FULL, 4, 1, 3, 0), (FULL, 4, 0, 3, 0),
        (DIAG, 4, 3, 3, 0), (FULL, 4, 2, 3, 1), (PROJECT, 2, 0, 0, 0), (PROJECT, 3, 0, 0, 0)],
    1: _diag(1, range(4)) + [(FULL, 0, 0, 0, 1), (FULL, 1, 0, 1, 1), (PROJECT, 0, 0, 0, 0), (FULL, 2, 0, 2, 1), (PROJECT, 1, 0, 0, 0),
        (FULL, 3, 0, 3, 1), (PROJECT, 2, 0, 0, 0), (PROJECT, 3, 0, 0, 0)],
    2: _diag(2, range(4)) + [(FULL, 0, 1, 0, 0), (FULL, 1, 1, 1, 0), (FULL, 0, 0, 0, 1), (FULL, 1, 0, 1, 1), (PROJECT, 0, 0, 0, 0),
        (FULL, 2, 1, 2, 0), (PROJECT, 1, 0, 0, 0), (FULL, 2, 0, 2, 1), (FULL, 3, 1, 3, 0), (PROJECT, 2, 0, 0, 0), (FULL, 3, 0, 3, 1),
        (PROJECT, 3, 0, 0, 0)],
    3: _diag(3, range(3)) + [(FULL, 0, 2, 0, 0), (FULL, 0, 0, 0, 0), (FULL, 1, 2, 1, 0), (FULL, 1, 0, 1, 0), (FULL, 2, 0, 2, 0),
        (FULL, 2, 2, 2, 0), (FULL, 0, 1, 0, 1), (FULL, 1, 1, 1, 1), (PROJECT, 0, 0, 0, 0), (PROJECT, 1, 0, 0, 0), (FULL, 2, 1, 2, 1),
        (PROJECT, 2, 0, 0, 0), (PROJECT, 3, 0, 0, 0)],
}
N_TASKS = max(len(t) for t in TASKS.values())
Q_WAIT = 6

SENDS = {p: [] for p in range(4)}
for (_p, _s), _to in AFTER_KV.items():
    SENDS[_p] += [(t, _p, _s, i) for t in _to for i in range(2)]
for _table in (PASS_Q, PASS_T):
    for (_p, _), _list in _table.items():
        SENDS[_p] += _list
_early = {p: {m[1:] for m in SENDS[p] if m[1] != p} for p in range(4)}
for _p, _table in PASS_IN.items():
    SENDS[_p] += [(to, j, s, i) for (j, s), to in _table.items() for i in range(2) if (j, s, i) not in _early[_p]]
N_SENDS = max(len(v) for v in SENDS.values())


def _task_waits(p):
    return [(n, i, j, s, PASS_IN[p].get((j, s))) for n, (kind, _, j, s, _) in enumerate(TASKS[p]) if kind != PROJECT and j != p
            for i in range(2) if (j, s, i) not in _early[p]]


def _pick(chip, step, table):
    out = jnp.int32(0)
    for p, row in table.items():
        for n, v in enumerate(row):
            if v:
                out = jnp.where((chip == p) & (step == n), jnp.int32(v), out)
    return out


def _dot(a, b, ca, cb):
    return lax.dot_general(a, b, (((ca,), (cb,)), ((), ())), preferred_element_type=jnp.float32)


def _kernel(x_ref, gain_ref, speed_ref, wq_ref, wk_ref, wv_ref, wo_ref, y_ref, a, w, q, kv, mix, top, ofin, osend, acc, cos, sin,
            w_sem, wo_sem, x_sem, out_sem, a_sem, kv_send, kv_recv, q_sem, o_send, o_recv):
    own, depth = x_ref.shape
    tokens = 2 * own
    me = lax.axis_index("sp")
    chip, core = lax.div(me, 2), lax.rem(me, 2)
    other = 2 * chip + 1 - core
    e = HEAD**-0.5 * LOG2E
    group = 8

    def half(h):
        return pl.ds(pl.multiple_of(h * own, own), own)

    def columns(n, width):
        return pl.ds(pl.multiple_of(n * width, width), width)

    def kv_weights(s):
        at, n = lax.rem(s, 2), core * SLOTS + s
        return (pltpu.make_async_copy(wk_ref.at[:, columns(n, HEAD)], w.at[at, :, pl.ds(0, HEAD)], w_sem.at[at]),
                pltpu.make_async_copy(wv_ref.at[:, columns(n, HEAD)], w.at[at, :, pl.ds(HEAD, HEAD)], w_sem.at[at]))

    def query_slot(i):
        return lax.rem(i + 3, SLOTS)

    def query_weights(i):
        at, n = lax.rem(i, 2), core * SLOTS + query_slot(i)
        return pltpu.make_async_copy(wq_ref.at[:, columns(n, 2 * HEAD)], w.at[at], w_sem.at[at])

    def out_slot(n):
        return jnp.where((chip == 3) & (n >= 2), 5 - n, n)

    def out_weights(n, k):
        head = jnp.where(k == 0, core, 1 - core) * SLOTS + out_slot(n)
        return pltpu.make_async_copy(wo_ref.at[columns(head, 2 * HEAD), :], a.at[half(k)], wo_sem.at[k])

    load_x = pltpu.make_async_copy(x_ref, a.at[half(core)], x_sem)
    load_x.start()
    for copy in kv_weights(0) + kv_weights(1):
        copy.start()

    barrier = pltpu.get_barrier_semaphore()
    for n in range(1, group):
        pl.semaphore_signal(barrier, inc=1, device_id={"sp": lax.rem(me + n, group)}, device_id_type=MESH)

    def rows_of(i):
        return pl.ds(pl.multiple_of(lax.rem(core + i, 2) * tokens, tokens), tokens)

    def send(p, m):
        to, j, s, i = m
        at, n = PLACE[to][j, s], SENDS[p].index(m)
        return pltpu.make_async_remote_copy(
            src_ref=kv.at[PLACE[p][j, s], rows_of(i)], dst_ref=kv.at[at, rows_of(i)], send_sem=kv_send.at[n],
            recv_sem=kv_recv.at[2 * (at - SLOTS) + i], device_id={"sp": 2 * to + core}, device_id_type=MESH)

    def arrived(p, j, s, i):
        at = PLACE[p][j, s]
        pltpu.make_async_remote_copy(
            src_ref=kv.at[at, rows_of(i)], dst_ref=kv.at[at, rows_of(i)], send_sem=kv_send.at[0],
            recv_sem=kv_recv.at[2 * (at - SLOTS) + i], device_id={"sp": other}, device_id_type=MESH).wait_recv()

    def on_chips(steps):
        for p, cases in steps.items():
            if cases:
                @pl.when(chip == p)
                def _(cases=cases):
                    for condition, action in cases:
                        pl.when(condition)(action)

    def pass_on(p, messages):
        for m in messages:
            arrived(p, *m[1:])
            send(p, m).start()

    def pass_steps(table, step):
        return {p: [(step == n, functools.partial(pass_on, p, messages)) for (c, n), messages in table.items() if c == p] for p in range(4)}

    send_a = pltpu.make_async_remote_copy(
        src_ref=a.at[half(core)], dst_ref=a.at[half(core)], send_sem=a_sem.at[0], recv_sem=a_sem.at[1],
        device_id={"sp": other}, device_id_type=MESH)
    recv_a = pltpu.make_async_remote_copy(
        src_ref=a.at[half(1 - core)], dst_ref=a.at[half(1 - core)], send_sem=a_sem.at[0], recv_sem=a_sem.at[1],
        device_id={"sp": other}, device_id_type=MESH)
    send_q = pltpu.make_async_remote_copy(
        src_ref=q.at[AWAY], dst_ref=q.at[SLOTS], send_sem=q_sem.at[0], recv_sem=q_sem.at[1],
        device_id={"sp": core}, device_id_type=MESH)

    def send_o(source, head, to):
        return pltpu.make_async_remote_copy(
            src_ref=osend.at[source], dst_ref=ofin.at[:, columns(head, 2 * HEAD)], send_sem=o_send.at[source],
            recv_sem=o_recv.at[head], device_id={"sp": to}, device_id_type=MESH)

    def o_arrived(head):
        pltpu.make_async_remote_copy(
            src_ref=osend.at[0], dst_ref=ofin.at[:, columns(head, 2 * HEAD)], send_sem=o_send.at[0],
            recv_sem=o_recv.at[head], device_id={"sp": other}, device_id_type=MESH).wait_recv()

    top[...] = jnp.full(top.shape, NEG, jnp.float32)

    def table(i, _):
        n = 64
        here = pl.ds(pl.multiple_of(i * n, n), n)
        place = chip * tokens + i * n + lax.broadcasted_iota(jnp.int32, (n, HEAD // 2), 0)
        angle = place.astype(jnp.float32) * speed_ref[...]
        cos[here, :] = jnp.cos(angle)
        sin[here, :] = jnp.sin(angle)

    lax.fori_loop(0, tokens // 64, table, None)
    load_x.wait()
    rows = 16

    def norm(i, _):
        here = pl.ds(pl.multiple_of(core * own + i * rows, rows), rows)
        wide = a[here, :].astype(jnp.float32)
        acc[pl.ds(pl.multiple_of(i * rows, rows), rows), :] = wide
        scale = lax.rsqrt(jnp.mean(wide * wide, -1, keepdims=True) + 1e-6)
        a[here, :] = (wide * scale * gain_ref[...].astype(jnp.float32)).astype(a.dtype)

    lax.fori_loop(0, own // rows, norm, None)
    pl.semaphore_wait(barrier, group - 1)
    send_a.start()

    def turned(t, cos, sin):
        t = t.astype(jnp.bfloat16).astype(jnp.float32)
        u, v = t[:, : HEAD // 2], t[:, HEAD // 2 :]
        return jnp.concatenate([u * cos - v * sin, v * cos + u * sin], -1).astype(jnp.bfloat16)

    def kv_step(n, _):
        s = jnp.where(n < 4, lax.rem(n, 2), lax.div(n, 2))
        i = jnp.where(n < 4, lax.div(n, 2), lax.rem(n, 2))
        h, at = lax.rem(core + i, 2), lax.rem(s, 2)

        @pl.when(i == 0)
        def _():
            for copy in kv_weights(s):
                copy.wait()

        @pl.when(n == 2)
        def _():
            recv_a.wait_recv()

        got = jnp.dot(a[half(h), :], w[at], preferred_element_type=jnp.float32)
        kv[s, pl.ds(pl.multiple_of(h * tokens, own), own), :] = turned(got[:, :HEAD], cos[half(h), :], sin[half(h), :])
        values = got[:, HEAD:].astype(jnp.bfloat16).T
        for b in range(own // HEAD):
            place = pl.ds(pl.multiple_of(h * tokens + own + b * HEAD, HEAD), HEAD)
            kv[s, place, :] = values[:, b * HEAD : (b + 1) * HEAD]

        @pl.when((i == 1) & (s < SLOTS - 2))
        def _():
            for copy in kv_weights(s + 2):
                copy.start()

        @pl.when((i == 1) & (s >= SLOTS - 2))
        def _():
            query_weights(s - (SLOTS - 2)).start()

        def go(p, s, half):
            for to in AFTER_KV[p, s]:
                send(p, (to, p, s, half)).start()

        on_chips({p: [((s == c) & (i == k), functools.partial(go, p, c, k)) for (o, c) in AFTER_KV if o == p for k in range(2)]
                  for p in range(4)})

    lax.fori_loop(0, 2 * SLOTS, kv_step, None)

    def q_step(i, _):
        at = lax.rem(i, 2)
        s = query_slot(i)
        query_weights(i).wait()

        def part(h, _):
            got = jnp.dot(a[half(h), :], w[at], preferred_element_type=jnp.float32)
            for g in range(2):
                place = pl.ds(pl.multiple_of(g * tokens + h * own, own), own)
                q[s, place, :] = turned(got[:, g * HEAD : (g + 1) * HEAD], cos[half(h), :], sin[half(h), :])

        lax.fori_loop(0, 2, part, None)

        @pl.when(i < SLOTS - 2)
        def _():
            query_weights(i + 2).start()

        @pl.when((i == 0) & (chip == 3))
        def _():
            send_q.start()

        on_chips(pass_steps(PASS_Q, i))

    lax.fori_loop(0, SLOTS, q_step, None)
    send_a.wait_send()
    for k in range(2):
        out_weights(0, k).start()
    mix[...] = jnp.zeros(mix.shape, jnp.float32)

    strip = own
    n_strips = 2 * tokens // strip
    ones = jnp.ones((8, strip), jnp.bfloat16)

    def block(qs, at, h, strips):
        keys = kv[at, pl.ds(pl.multiple_of(h * tokens, strip), strip), :]
        values = [kv[at, pl.ds(pl.multiple_of(h * tokens + own + b * HEAD, HEAD), HEAD), :] for b in range(strip // HEAD)]
        values = jnp.concatenate([jnp.concatenate(values, axis=1), ones], axis=0)
        spans = [pl.ds(n * strip, strip) for n, _ in strips]
        scores = [_dot(keys, q[qs, span, :], 1, 1) for span in spans]
        weights, keeps = [], []
        for (_, masked), span, s in zip(strips, spans, scores):
            if masked:
                seen = lax.broadcasted_iota(jnp.int32, s.shape, 1) >= lax.broadcasted_iota(jnp.int32, s.shape, 0)
                s = jnp.where(seen, s, HIDDEN)
            old = top[qs, :, span]
            new = jnp.maximum(old, s.max(axis=0, keepdims=True))
            top[qs, :, span] = new
            weights.append(jnp.exp2((s - new) * e).astype(jnp.bfloat16))
            keeps.append(jnp.exp2((old - new) * e))
        for span, p, keep in zip(spans, weights, keeps):
            mix[qs, :, span] = mix[qs, :, span] * keep + _dot(values, p, 1, 0)

    def finish(qs):
        def part(h, _):
            local = (h == core) & (qs < SLOTS)
            source = jnp.where(qs < SLOTS, qs, SLOTS + h)
            for g in range(2):
                span = pl.ds(pl.multiple_of(g * tokens + h * own, own), own)
                out = (mix[qs, :HEAD, span] * (1 / mix[qs, HEAD : HEAD + 1, span])).T.astype(jnp.bfloat16)

                @pl.when(local)
                def _():
                    ofin[:, pl.ds(pl.multiple_of((core * SLOTS + qs) * 2 * HEAD + g * HEAD, HEAD), HEAD)] = out

                @pl.when(jnp.logical_not(local))
                def _():
                    osend[source, :, g * HEAD : (g + 1) * HEAD] = out

        lax.fori_loop(0, 2, part, None)

        @pl.when(qs < SLOTS)
        def _():
            send_o(qs, core * SLOTS + qs, other).start()

        @pl.when(qs == SLOTS)
        def _():
            for h in range(2):
                send_o(SLOTS + h, core * SLOTS + AWAY, 6 + h).start()

    wide = 3 * HEAD

    def put(t):
        return pltpu.make_async_copy(q.at[t // 4, pl.ds(t % 4 * own, own), :], y_ref.at[:, pl.ds(t * HEAD, HEAD)], out_sem.at[t])

    def project(n):
        s = out_slot(n)
        o_arrived((1 - core) * SLOTS + s)

        @pl.when((chip == 3) & (s == AWAY))
        def _():
            o_arrived(core * SLOTS + AWAY)

        for k in range(2):
            out_weights(n, k).wait()

        def tile(t):
            here = pl.ds(pl.multiple_of(t * wide, wide), wide)
            left = jnp.concatenate([ofin[:, columns(c * SLOTS + s, 2 * HEAD)] for c in (core, 1 - core)], axis=1)
            return acc[:, here] + jnp.dot(left, a[:, here], preferred_element_type=jnp.float32), here

        @pl.when(n < SLOTS - 1)
        def _():
            def add(t, _):
                got, here = tile(t)
                acc[:, here] = got

            lax.fori_loop(0, depth // wide, add, None)
            for k in range(2):
                out_weights(n + 1, k).start()

        @pl.when(n == SLOTS - 1)
        def _():
            def last(t, _):
                got, _ = tile(t)
                for b in range(wide // HEAD):
                    m = t * (wide // HEAD) + b
                    at = pl.ds(pl.multiple_of(lax.rem(m, 4) * own, own), own)
                    q[lax.div(m, 4), at, :] = got[:, b * HEAD : (b + 1) * HEAD].astype(q.dtype)
                    pltpu.make_async_copy(q.at[lax.div(m, 4), at, :], y_ref.at[:, columns(m, HEAD)], out_sem.at[m]).start()

            lax.fori_loop(0, depth // wide, last, None)

    kind_of = {p: [t[0] for t in ts] for p, ts in TASKS.items()}
    slot_of = {p: [t[1] for t in ts] for p, ts in TASKS.items()}
    place_of = {p: [PLACE[p].get(t[2:4], 0) for t in ts] for p, ts in TASKS.items()}
    ends = {p: [t[4] for t in ts] for p, ts in TASKS.items()}

    def task(n, _):
        on_chips(pass_steps(PASS_T, n))

        @pl.when((chip == 0) & (n == Q_WAIT))
        def _():
            send_q.wait_recv()

        kind, qs, at, end = (_pick(chip, n, t) for t in (kind_of, slot_of, place_of, ends))

        def take(p, j, s, i, to):
            arrived(p, j, s, i)
            if to is not None:
                send(p, (to, j, s, i)).start()

        def part(i, _):
            on_chips({p: [((n == t) & (i == k), functools.partial(take, p, j, s, k, to)) for t, k, j, s, to in _task_waits(p)]
                      for p in range(4)})

            @pl.when(kind == FULL)
            def _():
                block(qs, at, lax.rem(core + i, 2), [(m, False) for m in range(n_strips)])

        @pl.when((kind == FULL) | (kind == DIAG))
        def _():
            lax.fori_loop(0, 2, part, None)

        @pl.when(kind == DIAG)
        def _():
            block(qs, at, 0, [(0, True), (1, False), (2, True), (3, False)])
            block(qs, at, 1, [(1, True), (3, True)])

        @pl.when(end == 1)
        def _():
            finish(qs)

        @pl.when(kind == PROJECT)
        def _():
            @pl.when((chip == 3) & (qs == SLOTS - 1))
            def _():
                send_q.wait_send()

            project(qs)

    lax.fori_loop(0, N_TASKS, task, None)

    for p in range(4):
        @pl.when(chip == p)
        def _(p=p):
            for m in SENDS[p]:
                send(p, m).wait_send()
    for s in range(SLOTS - 1):
        send_o(s, core * SLOTS + s, other).wait_send()

    @pl.when(chip != 3)
    def _():
        send_o(AWAY, core * SLOTS + AWAY, other).wait_send()

    @pl.when(chip == 0)
    def _():
        for h in range(2):
            send_o(SLOTS + h, core * SLOTS + AWAY, 6 + h).wait_send()

    for t in range(depth // HEAD):
        put(t).wait()


def layer(x, gain, wq, wk, wv, wo):
    own, depth = x.shape
    tokens = 2 * own
    low, f32 = jnp.bfloat16, jnp.float32
    anywhere, vmem = pl.BlockSpec(memory_space=pl.ANY), pl.BlockSpec(memory_space=pltpu.VMEM)
    dma = pltpu.SemaphoreType.DMA
    n = HEAD // 2
    speed = jnp.asarray(np.float32(THETA) ** (-np.arange(n, dtype=np.float32) / np.float32(n)))[None]
    return pl.pallas_call(
        _kernel,
        out_shape=jax.ShapeDtypeStruct(x.shape, low),
        in_specs=[anywhere, vmem, vmem, anywhere, anywhere, anywhere, anywhere],
        out_specs=anywhere,
        scratch_shapes=[
            pltpu.VMEM((tokens, depth), low),
            pltpu.VMEM((2, depth, 2 * HEAD), low),
            pltpu.VMEM((SLOTS + 1, 2 * tokens, HEAD), low),
            pltpu.VMEM((N_KV, 2 * tokens, HEAD), low),
            pltpu.VMEM((SLOTS + 1, HEAD + 8, 2 * tokens), f32),
            pltpu.VMEM((SLOTS + 1, 1, 2 * tokens), f32),
            pltpu.VMEM((own, wq.shape[1]), low),
            pltpu.VMEM((SLOTS + 2, own, 2 * HEAD), low),
            pltpu.VMEM((own, depth), f32),
            pltpu.VMEM((tokens, n), f32),
            pltpu.VMEM((tokens, n), f32),
            dma((2,)), dma((2,)), dma(()), dma((depth // HEAD,)), dma((2,)), dma((N_SENDS,)), dma((2 * (N_KV - SLOTS),)), dma((2,)),
            dma((SLOTS + 2,)), dma((2 * SLOTS,)),
        ],
        compiler_params=pltpu.CompilerParams(collective_id=0, has_side_effects=True, vmem_limit_bytes=67043328),
        cost_estimate=pl.CostEstimate(flops=66 * 10**9, bytes_accessed=70 * 10**6, transcendentals=20 * 10**6),
    )(x, gain[None], speed, wq, wk, wv, wo)


def solution(mesh):
    tokens, whole = P(("dp", "sp"), None), P(None, None)
    return jax.shard_map(
        layer,
        mesh=mesh,
        in_specs=(tokens, P(None), whole, whole, whole, whole),
        out_specs=tokens,
        check_vma=False,
    )
```

```python
import functools

import jax
import jax.numpy as jnp
import numpy as np
from jax import lax
from jax.experimental import pallas as pl
from jax.experimental.pallas import tpu as pltpu
from jax.sharding import PartitionSpec as P

HEAD = 256
THETA = 10000
NEG = -1e30
HIDDEN = 2 * NEG
LOG2E = 1.4426950408889634
MESH = pl.DeviceIdType.MESH
SLOTS = 4
NONE, FULL, DIAG, PROJECT = 0, 1, 2, 3
CHIPS, CORES = 4, 2
LENT = {3: ((0, 1), (0,)), 2: ((0,), (0,))}
HOST = {3: 0, 2: 1}

AFTER_KV = {
    (0, 0): {s: (1, 3) if s > 1 else (1,) for s in range(4)},
    (0, 1): {s: (1, 3) if s > 0 else (1,) for s in range(4)},
    (1, 0): {0: (0,), 1: (2, 0), 2: (2,), 3: (2,)},
    (1, 1): {0: (0,), 1: (2,), 2: (2,), 3: (2,)},
    (2, 0): {0: (1,), 1: (1,), 2: (3,)},
    (2, 1): {0: (1,), 1: (3,), 2: (3,)},
    (3, 0): {0: (0,), 1: (0,)},
    (3, 1): {0: (0,)},
}
PASS_Q = {
    (1, 0): {2: [(2, 0, 1, 0)], 3: [(0, 2, 0, 0), (0, 2, 0, 1), (2, 0, 1, 1)]},
    (1, 1): {0: [(0, 2, 0, 0)], 1: [(0, 1, 2, 1), (0, 2, 0, 1)]},
    (2, 0): {0: [(3, 1, 2, 0), (3, 2, 3, 1)], 2: [(3, 2, 3, 0)], 3: [(3, 1, 2, 1)]},
    (2, 1): {0: [(3, 1, 1, 0)], 1: [(3, 1, 2, 0)]},
    (3, 0): {0: [(2, 0, 2, 0)], 1: [(2, 0, 2, 1)]},
    (3, 1): {0: [(2, 0, 2, 0)], 3: [(2, 0, 2, 1)]},
}
PASS_T = {
    (0, 1): {4: [(3, 1, 2, 1)], 8: [(3, 1, 3, 1)]},
    (1, 0): {0: [(0, 2, 1, 0)], 3: [(0, 2, 1, 1)]},
    (1, 1): {3: [(0, 1, 3, 1)]},
    (2, 1): {1: [(3, 1, 1, 1)], 5: [(3, 2, 3, 0)], 6: [(3, 2, 3, 1)]},
    (3, 1): {1: [(2, 0, 1, 0)], 2: [(2, 0, 1, 1)]},
}
PASS_IN = {
    (2, 0): {(1, 3, 0): 3, (1, 3, 1): 3},
    (2, 1): {(1, 3, 0): 3},
    (3, 0): {(0, 3, 0): 2, (0, 3, 1): 2},
    (3, 1): {(0, 3, 0): 2, (0, 3, 1): 2},
}
ROLES = [(p, c) for p in range(CHIPS) for c in range(CORES)]

TASKS = {
    (0, 0): [
        (DIAG, 2, 2, 0, 2, 1, 0), (DIAG, 3, 3, 0, 3, 1, 0), (PROJECT, 0, 0, 0, 0, 0, 0), (PROJECT, 1, 0, 0, 0, 0, 0),
        (DIAG, 0, 0, 0, 0, 1, 0), (FULL, 4, 4, 0, 0, 0, 0), (FULL, 4, 4, 1, 0, 0, 0), (DIAG, 1, 1, 0, 1, 1, 0),
        (FULL, 4, 4, 2, 0, 0, 0), (DIAG, 4, 4, 3, 0, 1, 0), (FULL, 5, 0, 0, 1, 0, 1), (FULL, 5, 0, 1, 1, 0, 0),
        (FULL, 5, 0, 2, 1, 0, 0), (DIAG, 5, 0, 3, 1, 1, 0), (PROJECT, 2, 0, 0, 0, 0, 0), (PROJECT, 3, 0, 0, 0, 0, 0),
    ],
    (0, 1): [
        (DIAG, 2, 2, 0, 2, 1, 0), (DIAG, 3, 3, 0, 3, 1, 0), (FULL, 4, 4, 1, 0, 0, 0), (FULL, 4, 4, 0, 0, 0, 0),
        (DIAG, 4, 4, 3, 0, 0, 0), (FULL, 4, 4, 2, 0, 1, 0), (PROJECT, 0, 0, 0, 0, 0, 0), (PROJECT, 1, 0, 0, 0, 0, 0),
        (DIAG, 1, 1, 0, 1, 1, 0), (DIAG, 0, 0, 0, 0, 1, 0), (PROJECT, 2, 0, 0, 0, 0, 0), (PROJECT, 3, 0, 0, 0, 0, 0),
    ],
    (1, 0): [
        (DIAG, 1, 1, 1, 1, 0, 0), (FULL, 1, 1, 0, 1, 1, 0), (PROJECT, 0, 0, 0, 0, 0, 0), (DIAG, 0, 0, 1, 0, 0, 0),
        (FULL, 4, 4, 1, 0, 0, 0), (DIAG, 4, 4, 2, 0, 0, 0), (FULL, 0, 0, 0, 0, 1, 0), (FULL, 4, 4, 0, 0, 1, 0),
        (DIAG, 2, 2, 1, 2, 0, 0), (FULL, 2, 2, 0, 2, 1, 0), (PROJECT, 1, 0, 0, 0, 0, 0), (PROJECT, 2, 0, 0, 0, 0, 0),
        (FULL, 3, 3, 0, 3, 0, 0), (DIAG, 3, 3, 1, 3, 1, 0), (PROJECT, 3, 0, 0, 0, 0, 0),
    ],
    (1, 1): [
        (DIAG, 1, 1, 1, 1, 0, 0), (FULL, 1, 1, 0, 1, 1, 0), (DIAG, 3, 3, 1, 3, 0, 0), (DIAG, 2, 2, 1, 2, 0, 0),
        (FULL, 4, 4, 1, 0, 0, 0), (DIAG, 4, 4, 2, 0, 0, 0), (PROJECT, 0, 0, 0, 0, 0, 0), (DIAG, 0, 0, 1, 0, 0, 0),
        (FULL, 0, 0, 0, 0, 1, 0), (PROJECT, 1, 0, 0, 0, 0, 0), (FULL, 2, 2, 0, 2, 1, 0), (FULL, 4, 4, 0, 0, 1, 0),
        (PROJECT, 2, 0, 0, 0, 0, 0), (FULL, 3, 3, 0, 3, 1, 0), (PROJECT, 3, 0, 0, 0, 0, 0),
    ],
    (2, 0): [
        (DIAG, 1, 1, 2, 1, 0, 0), (FULL, 2, 2, 0, 2, 0, 0), (FULL, 2, 2, 1, 2, 0, 0), (FULL, 3, 3, 0, 3, 0, 0),
        (DIAG, 2, 2, 2, 2, 1, 0), (FULL, 3, 3, 1, 3, 0, 0), (FULL, 1, 1, 1, 1, 0, 0), (PROJECT, 0, 0, 0, 0, 0, 0),
        (FULL, 1, 1, 0, 1, 1, 0), (DIAG, 3, 3, 2, 3, 1, 0), (PROJECT, 1, 0, 0, 0, 0, 0), (PROJECT, 2, 0, 0, 0, 0, 0),
        (PROJECT, 3, 0, 0, 0, 0, 0),
    ],
    (2, 1): [
        (DIAG, 3, 3, 2, 3, 0, 0), (FULL, 2, 2, 1, 2, 0, 0), (FULL, 2, 2, 0, 2, 0, 0), (DIAG, 2, 2, 2, 2, 1, 0),
        (FULL, 1, 1, 0, 1, 0, 0), (DIAG, 1, 1, 2, 1, 0, 0), (FULL, 1, 1, 1, 1, 1, 0), (FULL, 3, 3, 0, 3, 0, 0),
        (FULL, 3, 3, 1, 3, 1, 0), (PROJECT, 0, 0, 0, 0, 0, 0), (PROJECT, 1, 0, 0, 0, 0, 0), (PROJECT, 2, 0, 0, 0, 0, 0),
        (PROJECT, 3, 0, 0, 0, 0, 0),
    ],
    (3, 0): [
        (FULL, 3, 3, 0, 3, 0, 0), (DIAG, 3, 3, 3, 3, 0, 0), (FULL, 2, 2, 2, 2, 0, 0), (FULL, 3, 3, 2, 3, 0, 0),
        (DIAG, 2, 2, 3, 2, 0, 0), (FULL, 2, 2, 0, 2, 0, 0), (FULL, 2, 2, 1, 2, 1, 0), (PROJECT, 0, 0, 0, 0, 0, 0),
        (PROJECT, 1, 0, 0, 0, 0, 0), (FULL, 3, 3, 1, 3, 1, 0), (PROJECT, 2, 0, 0, 0, 0, 0), (PROJECT, 3, 0, 0, 0, 0, 0),
    ],
    (3, 1): [
        (DIAG, 3, 3, 3, 3, 0, 0), (FULL, 1, 1, 2, 1, 0, 0), (FULL, 1, 1, 0, 1, 0, 0), (DIAG, 1, 1, 3, 1, 0, 0),
        (FULL, 3, 3, 0, 3, 0, 0), (FULL, 1, 1, 1, 1, 1, 0), (FULL, 2, 2, 1, 2, 0, 0), (FULL, 2, 2, 2, 2, 0, 0),
        (FULL, 2, 2, 0, 2, 0, 0), (DIAG, 2, 2, 3, 2, 1, 0), (PROJECT, 0, 0, 0, 0, 0, 0), (PROJECT, 1, 0, 0, 0, 0, 0),
        (FULL, 3, 3, 2, 3, 0, 0), (PROJECT, 2, 0, 0, 0, 0, 0), (FULL, 3, 3, 1, 3, 1, 0), (PROJECT, 3, 0, 0, 0, 0, 0),
    ],
}
N_TASKS = max(len(t) for t in TASKS.values())
KV_ORDER = {0: (1, 2, 0, 3), 1: (0, 1, 2, 3), 2: (2, 0, 1, 3), 3: (0, 3, 2, 1)}
OUT_ORDER = {0: (2, 3, 0, 1), 1: (1, 0, 2, 3), 2: (2, 3, 1, 0), 3: (2, 0, 1, 3)}

SENDS = {r: [(to, r[0], s, i) for s, tos in AFTER_KV[r].items() for to in tos for i in range(2)] for r in ROLES}
for _table in (PASS_Q, PASS_T):
    for _r, _steps in _table.items():
        SENDS[_r] += [m for messages in _steps.values() for m in messages]
_early = {r: {m[1:] for m in SENDS[r] if m[1] != r[0]} for r in ROLES}
for _r, _table in PASS_IN.items():
    SENDS[_r] += [(to, *m) for m, to in _table.items() if m not in _early[_r]]
N_SENDS = max(len(v) for v in SENDS.values())

PLACE = {r: {(r[0], s): s for s in range(SLOTS)} for r in ROLES}
for _p, _c in ROLES:
    for _to, _j, _s, _ in SENDS[_p, _c]:
        PLACE[_to, _c].setdefault((_j, _s), len(PLACE[_to, _c]))
N_KV = max(len(v) for v in PLACE.values())


def _task_waits(r):
    waits, seen = [], set(_early[r])
    for n, (kind, _, _, j, s, _, _) in enumerate(TASKS[r]):
        for i in range(2):
            if kind != PROJECT and j != r[0] and (j, s, i) not in seen:
                seen.add((j, s, i))
                waits.append((n, i, j, s, PASS_IN.get(r, {}).get((j, s, i))))
    return waits


def _query_waits(r):
    first = {}
    for n, (kind, at, *_) in enumerate(TASKS[r]):
        if kind != PROJECT and at >= SLOTS:
            first.setdefault(at, n)
    return [(n, at) for at, n in first.items()]


def _check():
    got = {r: set() for r in ROLES}
    for p, c in ROLES:
        for to, j, s, i in SENDS[p, c]:
            assert (j, s, i) not in got[to, c]
            got[to, c].add((j, s, i))
    for r in ROLES:
        need = {(j, s, i) for kind, _, _, j, s, _, _ in TASKS[r] if kind != PROJECT and j != r[0] for i in range(2)}
        assert got[r] == need | _early[r], r


_check()


def _pick(row, step, table):
    out = jnp.int32(0)
    for r, values in table.items():
        here = jnp.int32(0)
        for n, v in enumerate(values):
            if v:
                here = jnp.where(step == n, jnp.int32(v), here)
        out = jnp.where(row == r, here, out)
    return out


def _osend(s, h):
    n = SLOTS + 2 * s + h
    return n - SLOTS * (n // (SLOTS + 3))


def _dot(a, b, ca, cb):
    return lax.dot_general(a, b, (((ca,), (cb,)), ((), ())), preferred_element_type=jnp.float32)


def _kernel(x_ref, gain_ref, speed_ref, wq_ref, wk_ref, wv_ref, wo_ref, y_ref, a, w, q, kv, mix, top, ofin, osend, acc, cos, sin, gain_s,
            w_sem, wo_sem, x_sem, out_sem, a_send, a_recv, kv_send, kv_recv, q_send, q_recv, o_send, o_recv):
    own, depth = x_ref.shape
    tokens = 2 * own
    me = lax.axis_index("sp")
    chip, core = lax.div(me, CORES), lax.rem(me, CORES)
    other = CORES * chip + 1 - core
    e = HEAD**-0.5 * LOG2E
    group = CHIPS * CORES

    def half(h):
        return pl.ds(pl.multiple_of(h * own, own), own)

    def columns(n, width):
        return pl.ds(pl.multiple_of(n * width, width), width)

    def kv_weights(m):
        at, n = lax.rem(jnp.int32(m), 2), core * SLOTS + _pick(chip, m, KV_ORDER)
        return (pltpu.make_async_copy(wk_ref.at[:, columns(n, HEAD)], w.at[at, :, pl.ds(0, HEAD)], w_sem.at[at]),
                pltpu.make_async_copy(wv_ref.at[:, columns(n, HEAD)], w.at[at, :, pl.ds(HEAD, HEAD)], w_sem.at[at]))

    def query_weights(s):
        at, n = lax.rem(s, 2), core * SLOTS + s
        return pltpu.make_async_copy(wq_ref.at[:, columns(n, 2 * HEAD)], w.at[at], w_sem.at[at])

    def out_slot(n):
        return _pick(chip, n, OUT_ORDER)

    wide = 5 * HEAD
    n_wide = depth // wide

    def out_weights(n, k, t):
        head = jnp.where(k == 0, core, 1 - core) * SLOTS + out_slot(n)
        return pltpu.make_async_copy(wo_ref.at[columns(head, 2 * HEAD), columns(t, wide)], a.at[half(k), columns(t, wide)], wo_sem.at[k, t])

    pieces = 4
    piece = own // pieces

    def rows_in(n, c):
        return pl.ds(pl.multiple_of(c * own + n * piece, piece), piece)

    def load_x(n):
        return pltpu.make_async_copy(x_ref.at[pl.ds(n * piece, piece), :], a.at[rows_in(n, core)], x_sem.at[n])

    def send_a(n, c=None):
        rows = rows_in(n, core if c is None else c)
        return pltpu.make_async_remote_copy(
            src_ref=a.at[rows], dst_ref=a.at[rows], send_sem=a_send.at[n], recv_sem=a_recv.at[n],
            device_id={"sp": other}, device_id_type=MESH)

    for n in range(pieces):
        load_x(n).start()

    barrier = pltpu.get_barrier_semaphore()
    for n in range(1, group):
        pl.semaphore_signal(barrier, inc=1, device_id={"sp": lax.rem(me + n, group)}, device_id_type=MESH)

    def rows_of(i):
        return pl.ds(pl.multiple_of(lax.rem(core + i, 2) * tokens, tokens), tokens)

    def send(r, m):
        to, j, s, i = m
        at, n = PLACE[to, r[1]][j, s], SENDS[r].index(m)
        return pltpu.make_async_remote_copy(
            src_ref=kv.at[PLACE[r][j, s], rows_of(i)], dst_ref=kv.at[at, rows_of(i)], send_sem=kv_send.at[n],
            recv_sem=kv_recv.at[2 * (at - SLOTS) + i], device_id={"sp": CORES * to + r[1]}, device_id_type=MESH)

    def arrived(r, j, s, i):
        at = PLACE[r][j, s]
        pltpu.make_async_remote_copy(
            src_ref=kv.at[at, rows_of(i)], dst_ref=kv.at[at, rows_of(i)], send_sem=kv_send.at[0],
            recv_sem=kv_recv.at[2 * (at - SLOTS) + i], device_id={"sp": other}, device_id_type=MESH).wait_recv()

    def by_role(cases):
        for (p, c), actions in cases.items():
            if actions:
                @pl.when(me == CORES * p + c)
                def _(actions=actions):
                    for condition, action in actions:
                        pl.when(condition)(action)

    def pass_on(r, messages):
        for m in messages:
            if m[1] != r[0]:
                arrived(r, *m[1:])
            send(r, m).start()

    def pass_steps(table, step):
        return {r: [(step == n, functools.partial(pass_on, r, messages)) for n, messages in steps.items()] for r, steps in table.items()}

    def send_q(s, to):
        return pltpu.make_async_remote_copy(
            src_ref=q.at[s], dst_ref=q.at[SLOTS + s], send_sem=q_send.at[s], recv_sem=q_recv.at[s],
            device_id={"sp": CORES * to + core}, device_id_type=MESH)

    def send_o(source, head, to):
        return pltpu.make_async_remote_copy(
            src_ref=osend.at[source], dst_ref=ofin.at[:, columns(head, 2 * HEAD)], send_sem=o_send.at[source],
            recv_sem=o_recv.at[head], device_id={"sp": to}, device_id_type=MESH)

    def o_arrived(head):
        send_o(0, head, other).wait_recv()

    def table(i, _):
        n = 64
        here = pl.ds(pl.multiple_of(i * n, n), n)
        place = chip * tokens + i * n + lax.broadcasted_iota(jnp.int32, (n, HEAD // 2), 0)
        angle = place.astype(jnp.float32) * speed_ref[...]
        cos[here, :] = jnp.cos(angle)
        sin[here, :] = jnp.sin(angle)

    lax.fori_loop(0, tokens // 64, table, None)
    gain_s[...] = gain_ref[...].astype(jnp.float32)[None]
    for copy in kv_weights(0) + kv_weights(1):
        copy.start()
    pl.semaphore_wait(barrier, group - 1)
    rows, together = 16, 4

    for n in range(pieces):
        load_x(n).wait()

        def norm(i, _, n=n):
            for k in range(together):
                at = n * piece + (i * together + k) * rows
                here = pl.ds(pl.multiple_of(core * own + at, rows), rows)
                wide = a[here, :].astype(jnp.float32)
                acc[pl.ds(pl.multiple_of(at, rows), rows), :] = wide
                scale = lax.rsqrt(jnp.mean(wide * wide, -1, keepdims=True) + 1e-6)
                a[here, :] = (wide * scale * gain_s[...]).astype(a.dtype)

        lax.fori_loop(0, piece // (rows * together), norm, None)
        send_a(n).start()

    def turned(t, cos, sin):
        t = t.astype(jnp.bfloat16).astype(jnp.float32)
        u, v = t[:, : HEAD // 2], t[:, HEAD // 2 :]
        return jnp.concatenate([u * cos - v * sin, v * cos + u * sin], -1).astype(jnp.bfloat16)

    def kv_step(n, _):
        m = jnp.where(n < 4, lax.rem(n, 2), lax.div(n, 2))
        i = jnp.where(n < 4, lax.div(n, 2), lax.rem(n, 2))
        s, h, at = _pick(chip, m, KV_ORDER), lax.rem(core + i, 2), lax.rem(m, 2)

        @pl.when(i == 0)
        def _():
            for copy in kv_weights(m):
                copy.wait()

        @pl.when(n == 2)
        def _():
            for k in range(pieces):
                send_a(k, 1 - core).wait_recv()

        got = jnp.dot(a[half(h), :], w[at], preferred_element_type=jnp.float32)
        kv[s, pl.ds(pl.multiple_of(h * tokens, own), own), :] = turned(got[:, :HEAD], cos[half(h), :], sin[half(h), :])
        values = got[:, HEAD:].astype(jnp.bfloat16).T
        for b in range(own // HEAD):
            place = pl.ds(pl.multiple_of(h * tokens + own + b * HEAD, HEAD), HEAD)
            kv[s, place, :] = values[:, b * HEAD : (b + 1) * HEAD]

        @pl.when((i == 1) & (m < SLOTS - 2))
        def _():
            for copy in kv_weights(m + 2):
                copy.start()

        @pl.when((i == 1) & (m >= SLOTS - 2))
        def _():
            query_weights(m - (SLOTS - 2)).start()

        def go(r, s, half):
            for to in AFTER_KV[r][s]:
                send(r, (to, r[0], s, half)).start()

        by_role({r: [((s == c) & (i == k), functools.partial(go, r, c, k)) for c in steps for k in range(2)] for r, steps in AFTER_KV.items()})

    lax.fori_loop(0, 2 * SLOTS, kv_step, None)

    def q_step(s, _):
        at = lax.rem(s, 2)
        query_weights(s).wait()
        for h in range(2):
            for g in range(2):
                got = jnp.dot(a[half(h), :], w[at, :, g * HEAD : (g + 1) * HEAD], preferred_element_type=jnp.float32)
                q[s, pl.ds(g * tokens + h * own, own), :] = turned(got, cos[half(h), :], sin[half(h), :])

        @pl.when(s < SLOTS - 2)
        def _():
            query_weights(s + 2).start()

        by_role({(p, c): [(s == k, functools.partial(lambda k, p: send_q(k, HOST[p]).start(), k, p)) for k in lent[c]]
                 for p, lent in LENT.items() for c in range(CORES)})
        by_role(pass_steps(PASS_Q, s))

    lax.fori_loop(0, SLOTS, q_step, None)
    for n in range(pieces):
        send_a(n).wait_send()
    for t in range(n_wide):
        for k in range(2):
            out_weights(0, k, t).start()

    def start_anew(state):
        top[state] = jnp.full(top.shape[1:], NEG, jnp.float32)
        mix[state] = jnp.zeros(mix.shape[1:], jnp.float32)

    lax.fori_loop(0, SLOTS + 1, lambda i, _: start_anew(i), None)

    strip = own
    n_strips = 2 * tokens // strip
    ones = jnp.ones((8, strip), jnp.bfloat16)

    def block(qs, state, at, h, strips):
        keys = kv[at, pl.ds(pl.multiple_of(h * tokens, strip), strip), :]
        values = [kv[at, pl.ds(pl.multiple_of(h * tokens + own + b * HEAD, HEAD), HEAD), :] for b in range(strip // HEAD)]
        values = jnp.concatenate([jnp.concatenate(values, axis=1), ones], axis=0)
        spans = [pl.ds(n * strip, strip) for n, _ in strips]
        scores = [_dot(keys, q[qs, span, :], 1, 1) for span in spans]
        weights, keeps = [], []
        for (_, masked), span, s in zip(strips, spans, scores):
            if masked:
                seen = lax.broadcasted_iota(jnp.int32, s.shape, 1) >= lax.broadcasted_iota(jnp.int32, s.shape, 0)
                s = jnp.where(seen, s, HIDDEN)
            old = top[state, :, span]
            new = jnp.maximum(old, s.max(axis=0, keepdims=True))
            top[state, :, span] = new
            weights.append(jnp.exp2((s - new) * e).astype(jnp.bfloat16))
            keeps.append(jnp.exp2((old - new) * e))
        for span, p, keep in zip(spans, weights, keeps):
            mix[state, :, span] = mix[state, :, span] * keep + _dot(values, p, 1, 0)

    def finish(qs, state):
        lent = qs >= SLOTS
        to = CORES * jnp.where(chip == HOST[3], 3, 2)

        @pl.when(qs > SLOTS)
        def _():
            send_o(SLOTS - 1, core * SLOTS + SLOTS - 1, other).wait_send()

        def part(m, _):
            h = lax.rem(core + 1 + m, 2)
            local = (h == core) & jnp.logical_not(lent)
            source = jnp.where(lent, _osend(qs - SLOTS, h), qs)
            for g in range(2):
                span = pl.ds(pl.multiple_of(g * tokens + h * own, own), own)
                out = (mix[state, :HEAD, span] * (1 / mix[state, HEAD : HEAD + 1, span])).T.astype(jnp.bfloat16)

                @pl.when(local)
                def _():
                    ofin[:, pl.ds(pl.multiple_of((core * SLOTS + qs) * 2 * HEAD + g * HEAD, HEAD), HEAD)] = out

                @pl.when(jnp.logical_not(local))
                def _():
                    osend[source, :, g * HEAD : (g + 1) * HEAD] = out

            @pl.when(lent)
            def _():
                send_o(source, core * SLOTS + qs - SLOTS, to + h).start()

            @pl.when(jnp.logical_not(lent) & (h != core))
            def _():
                send_o(source, core * SLOTS + qs, other).start()

        lax.fori_loop(0, 2, part, None)

    def project(n):
        s = out_slot(n)
        away = jnp.bool_(False)
        for p, lent in LENT.items():
            for c in range(CORES):
                for k in lent[c]:
                    away |= (me == CORES * p + c) & (s == k)

        def head(c):
            return ofin[:, columns(c * SLOTS + s, 2 * HEAD)]

        def part(t):
            return pl.ds(pl.multiple_of(t * wide, wide), wide)

        @pl.when(n < SLOTS - 1)
        def _():
            o_arrived((1 - core) * SLOTS + s)

            @pl.when(away)
            def _():
                o_arrived(core * SLOTS + s)

            def add(t, _):
                for k in range(2):
                    out_weights(n, k, t).wait()
                left = jnp.concatenate([head(core), head(1 - core)], axis=1)
                acc[:, part(t)] += jnp.dot(left, a[:, part(t)], preferred_element_type=jnp.float32)
                for k in range(2):
                    out_weights(n + 1, k, t).start()

            lax.fori_loop(0, n_wide, add, None)

        @pl.when(n == SLOTS - 1)
        def _():
            one = jnp.where(away, 1, 0)
            cores = [jnp.where(k == 0, core, 1 - core) for k in (one, 1 - one)]

            @pl.when(away)
            def _():
                o_arrived((1 - core) * SLOTS + s)

            def first(t, _):
                out_weights(n, one, t).wait()
                acc[:, part(t)] += jnp.dot(head(cores[0]), a[half(one), part(t)], preferred_element_type=jnp.float32)

            lax.fori_loop(0, n_wide, first, None)
            o_arrived(cores[1] * SLOTS + s)

            def last(t, _):
                out_weights(n, 1 - one, t).wait()
                got = acc[:, part(t)] + jnp.dot(head(cores[1]), a[half(1 - one), part(t)], preferred_element_type=jnp.float32)
                for b in range(wide // HEAD):
                    m = t * (wide // HEAD) + b
                    at = pl.ds(pl.multiple_of(lax.rem(m, 4) * own, own), own)
                    q[lax.div(m, 4), at, :] = got[:, b * HEAD : (b + 1) * HEAD].astype(q.dtype)
                    pltpu.make_async_copy(q.at[lax.div(m, 4), at, :], y_ref.at[:, columns(m, HEAD)], out_sem.at[m]).start()

            lax.fori_loop(0, n_wide, last, None)

    columns_of = [{CORES * p + c: [f(p, c, t) for t in TASKS[p, c]] for p, c in ROLES} for f in (
        lambda p, c, t: t[0], lambda p, c, t: t[1], lambda p, c, t: t[2], lambda p, c, t: PLACE[p, c].get(t[3:5], 0),
        lambda p, c, t: t[5], lambda p, c, t: t[6])]

    def task(n, _):
        by_role(pass_steps(PASS_T, n))
        by_role({r: [(n == t, functools.partial(lambda k: send_q(k, 0).wait_recv(), at - SLOTS)) for t, at in _query_waits(r)] for r in ROLES})
        kind, qs, state, at, end, reset = (_pick(me, n, t) for t in columns_of)

        @pl.when(reset == 1)
        def _():
            start_anew(state)

        def take(r, j, s, i, to):
            arrived(r, j, s, i)
            if to is not None:
                send(r, (to, j, s, i)).start()

        def part(i, _):
            by_role({r: [((n == t) & (i == k), functools.partial(take, r, j, s, k, to)) for t, k, j, s, to in _task_waits(r)] for r in ROLES})

            @pl.when(kind == FULL)
            def _():
                block(qs, state, at, lax.rem(core + i, 2), [(m, False) for m in range(n_strips)])

        @pl.when((kind == FULL) | (kind == DIAG))
        def _():
            lax.fori_loop(0, 2, part, None)

        @pl.when(kind == DIAG)
        def _():
            block(qs, state, at, 0, [(0, True), (1, False), (2, True), (3, False)])
            block(qs, state, at, 1, [(1, True), (3, True)])

        @pl.when(end == 1)
        def _():
            finish(qs, state)

        @pl.when(kind == PROJECT)
        def _():
            @pl.when(qs == SLOTS - 1)
            def _():
                for (p, c) in ROLES:
                    if p in LENT:
                        @pl.when(me == CORES * p + c)
                        def _(p=p, c=c):
                            for k in LENT[p][c]:
                                send_q(k, HOST[p]).wait_send()

            project(qs)

    lax.fori_loop(0, N_TASKS, task, None)

    for p, c in ROLES:
        @pl.when(me == CORES * p + c)
        def _(p=p, c=c):
            for m in SENDS[p, c]:
                send((p, c), m).wait_send()
            for s in range(SLOTS):
                again = s == SLOTS - 1 and any(host == p and len(LENT[guest][c]) > 1 for guest, host in HOST.items())
                if (p not in LENT or s not in LENT[p][c]) and not again:
                    send_o(s, c * SLOTS + s, other).wait_send()
            for guest, host in HOST.items():
                if host == p:
                    for s in LENT[guest][c]:
                        for h in range(2):
                            send_o(_osend(s, h), c * SLOTS + s, CORES * guest + h).wait_send()

    for m in range(depth // HEAD):
        pltpu.make_async_copy(q.at[m // 4, pl.ds(m % 4 * own, own), :], y_ref.at[:, pl.ds(m * HEAD, HEAD)], out_sem.at[m]).wait()


def _hand_over(y_ref, out_ref, held, sems):
    pieces = held.shape[0]

    def copies(n):
        rows = pl.ds(n * held.shape[1], held.shape[1])
        return (pltpu.make_async_copy(y_ref.at[rows, :], held.at[n], sems.at[0, n]),
                pltpu.make_async_copy(held.at[n], out_ref.at[rows, :], sems.at[1, n]))

    for n in range(pieces):
        copies(n)[0].start()
    for n in range(pieces):
        copies(n)[0].wait()
        copies(n)[1].start()
    for n in range(pieces):
        copies(n)[1].wait()


def hand_over(y):
    own, depth = y.shape
    pieces = 8
    anywhere = pl.BlockSpec(memory_space=pl.ANY)
    return pl.pallas_call(
        _hand_over,
        out_shape=jax.ShapeDtypeStruct(y.shape, y.dtype),
        in_specs=[anywhere],
        out_specs=anywhere,
        scratch_shapes=[pltpu.VMEM((pieces, own // pieces, depth), y.dtype), pltpu.SemaphoreType.DMA((2, pieces))],
        cost_estimate=pl.CostEstimate(flops=0, bytes_accessed=4 * own * depth, transcendentals=0),
    )(y)


def layer(x, gain, wq, wk, wv, wo):
    own, depth = x.shape
    tokens = 2 * own
    low, f32 = jnp.bfloat16, jnp.float32
    anywhere, vmem = pl.BlockSpec(memory_space=pl.ANY), pl.BlockSpec(memory_space=pltpu.VMEM)
    dma = pltpu.SemaphoreType.DMA
    n = HEAD // 2
    speed = jnp.asarray(np.float32(THETA) ** (-np.arange(n, dtype=np.float32) / np.float32(n)))[None]
    y = pl.pallas_call(
        _kernel,
        out_shape=jax.ShapeDtypeStruct(x.shape, low),
        in_specs=[anywhere, vmem, vmem, anywhere, anywhere, anywhere, anywhere],
        out_specs=anywhere,
        scratch_shapes=[
            pltpu.VMEM((tokens, depth), low),
            pltpu.VMEM((2, depth, 2 * HEAD), low),
            pltpu.VMEM((SLOTS + 2, 2 * tokens, HEAD), low),
            pltpu.VMEM((N_KV, 2 * tokens, HEAD), low),
            pltpu.VMEM((SLOTS + 1, HEAD + 8, 2 * tokens), f32),
            pltpu.VMEM((SLOTS + 1, 1, 2 * tokens), f32),
            pltpu.VMEM((own, wq.shape[1]), low),
            pltpu.VMEM((SLOTS + 3, own, 2 * HEAD), low),
            pltpu.VMEM((own, depth), f32),
            pltpu.VMEM((tokens, n), f32),
            pltpu.VMEM((tokens, n), f32),
            pltpu.VMEM((1, depth), f32),
            dma((2,)), dma((2, 3)), dma((4,)), dma((depth // HEAD,)), dma((4,)), dma((4,)), dma((N_SENDS,)), dma((2 * (N_KV - SLOTS),)),
            dma((2,)), dma((2,)), dma((SLOTS + 3,)), dma((2 * SLOTS,)),
        ],
        compiler_params=pltpu.CompilerParams(collective_id=0, has_side_effects=True, vmem_limit_bytes=67043328),
        cost_estimate=pl.CostEstimate(flops=66 * 10**9, bytes_accessed=70 * 10**6, transcendentals=20 * 10**6),
    )(x, gain, speed, wq, wk, wv, wo)
    return hand_over(y)


def solution(mesh):
    tokens, whole = P(("dp", "sp"), None), P(None, None)
    return jax.shard_map(
        layer,
        mesh=mesh,
        in_specs=(tokens, P(None), whole, whole, whole, whole),
        out_specs=tokens,
        check_vma=False,
    )
```

```python
import functools

import jax
import jax.numpy as jnp
import numpy as np
from jax import lax
from jax.experimental import pallas as pl
from jax.experimental.pallas import tpu as pltpu
from jax.sharding import PartitionSpec as P

HEAD = 256
THETA = 10000
NEG = -1e30
HIDDEN = 2 * NEG
LOG2E = 1.4426950408889634
MESH = pl.DeviceIdType.MESH
SLOTS = 4
NONE, FULL, DIAG, PROJECT = 0, 1, 2, 3
CHIPS, CORES = 4, 2
LENT = {3: ((0, 1), (0,)), 2: ((0,), (0,))}
HOST = {3: 0, 2: 1}

AFTER_KV = {
    (0, 0): {s: (1, 3) if s > 1 else (1,) for s in range(4)},
    (0, 1): {s: (1, 3) if s > 0 else (1,) for s in range(4)},
    (1, 0): {0: (0,), 1: (2, 0), 2: (2,), 3: (2,)},
    (1, 1): {0: (0,), 1: (2,), 2: (2,), 3: (2,)},
    (2, 0): {0: (1,), 1: (1,), 2: (3,)},
    (2, 1): {0: (1,), 1: (3,), 2: (3,)},
    (3, 0): {0: (0,), 1: (0,)},
    (3, 1): {0: (0,)},
}
PASS_Q = {
    (1, 0): {2: [(2, 0, 1, 0)], 3: [(0, 2, 0, 0), (0, 2, 0, 1), (2, 0, 1, 1)]},
    (1, 1): {0: [(0, 2, 0, 0)], 1: [(0, 1, 2, 1), (0, 2, 0, 1)]},
    (2, 0): {0: [(3, 1, 2, 0), (3, 2, 3, 1)], 2: [(3, 2, 3, 0)], 3: [(3, 1, 2, 1)]},
    (2, 1): {0: [(3, 1, 1, 0)], 1: [(3, 1, 2, 0)]},
    (3, 0): {0: [(2, 0, 2, 0)], 1: [(2, 0, 2, 1)]},
    (3, 1): {0: [(2, 0, 2, 0)], 3: [(2, 0, 2, 1)]},
}
PASS_T = {
    (0, 1): {4: [(3, 1, 2, 1)], 8: [(3, 1, 3, 1)]},
    (1, 0): {0: [(0, 2, 1, 0)], 3: [(0, 2, 1, 1)]},
    (1, 1): {3: [(0, 1, 3, 1)]},
    (2, 1): {1: [(3, 1, 1, 1)], 5: [(3, 2, 3, 0)], 6: [(3, 2, 3, 1)]},
    (3, 1): {1: [(2, 0, 1, 0)], 2: [(2, 0, 1, 1)]},
}
PASS_IN = {
    (2, 0): {(1, 3, 0): 3, (1, 3, 1): 3},
    (2, 1): {(1, 3, 0): 3},
    (3, 0): {(0, 3, 0): 2, (0, 3, 1): 2},
    (3, 1): {(0, 3, 0): 2, (0, 3, 1): 2},
}
ROLES = [(p, c) for p in range(CHIPS) for c in range(CORES)]

TASKS = {
    (0, 0): [
        (DIAG, 2, 2, 0, 2, 1, 0), (DIAG, 3, 3, 0, 3, 1, 0), (PROJECT, 0, 0, 0, 0, 0, 0), (PROJECT, 1, 0, 0, 0, 0, 0),
        (DIAG, 0, 0, 0, 0, 1, 0), (FULL, 4, 4, 0, 0, 0, 0), (FULL, 4, 4, 1, 0, 0, 0), (DIAG, 1, 1, 0, 1, 1, 0),
        (FULL, 4, 4, 2, 0, 0, 0), (DIAG, 4, 4, 3, 0, 1, 0), (FULL, 5, 0, 0, 1, 0, 1), (FULL, 5, 0, 1, 1, 0, 0),
        (FULL, 5, 0, 2, 1, 0, 0), (DIAG, 5, 0, 3, 1, 1, 0), (PROJECT, 2, 0, 0, 0, 0, 0), (PROJECT, 3, 0, 0, 0, 0, 0),
    ],
    (0, 1): [
        (DIAG, 2, 2, 0, 2, 1, 0), (DIAG, 3, 3, 0, 3, 1, 0), (FULL, 4, 4, 1, 0, 0, 0), (FULL, 4, 4, 0, 0, 0, 0),
        (DIAG, 4, 4, 3, 0, 0, 0), (FULL, 4, 4, 2, 0, 1, 0), (PROJECT, 0, 0, 0, 0, 0, 0), (PROJECT, 1, 0, 0, 0, 0, 0),
        (DIAG, 1, 1, 0, 1, 1, 0), (DIAG, 0, 0, 0, 0, 1, 0), (PROJECT, 2, 0, 0, 0, 0, 0), (PROJECT, 3, 0, 0, 0, 0, 0),
    ],
    (1, 0): [
        (DIAG, 1, 1, 1, 1, 0, 0), (FULL, 1, 1, 0, 1, 1, 0), (PROJECT, 0, 0, 0, 0, 0, 0), (DIAG, 0, 0, 1, 0, 0, 0),
        (FULL, 4, 4, 1, 0, 0, 0), (DIAG, 4, 4, 2, 0, 0, 0), (FULL, 0, 0, 0, 0, 1, 0), (FULL, 4, 4, 0, 0, 1, 0),
        (DIAG, 2, 2, 1, 2, 0, 0), (FULL, 2, 2, 0, 2, 1, 0), (PROJECT, 1, 0, 0, 0, 0, 0), (PROJECT, 2, 0, 0, 0, 0, 0),
        (FULL, 3, 3, 0, 3, 0, 0), (DIAG, 3, 3, 1, 3, 1, 0), (PROJECT, 3, 0, 0, 0, 0, 0),
    ],
    (1, 1): [
        (DIAG, 1, 1, 1, 1, 0, 0), (FULL, 1, 1, 0, 1, 1, 0), (DIAG, 3, 3, 1, 3, 0, 0), (DIAG, 2, 2, 1, 2, 0, 0),
        (FULL, 4, 4, 1, 0, 0, 0), (DIAG, 4, 4, 2, 0, 0, 0), (PROJECT, 0, 0, 0, 0, 0, 0), (DIAG, 0, 0, 1, 0, 0, 0),
        (FULL, 0, 0, 0, 0, 1, 0), (PROJECT, 1, 0, 0, 0, 0, 0), (FULL, 2, 2, 0, 2, 1, 0), (FULL, 4, 4, 0, 0, 1, 0),
        (PROJECT, 2, 0, 0, 0, 0, 0), (FULL, 3, 3, 0, 3, 1, 0), (PROJECT, 3, 0, 0, 0, 0, 0),
    ],
    (2, 0): [
        (DIAG, 1, 1, 2, 1, 0, 0), (FULL, 2, 2, 0, 2, 0, 0), (FULL, 2, 2, 1, 2, 0, 0), (FULL, 3, 3, 0, 3, 0, 0),
        (DIAG, 2, 2, 2, 2, 1, 0), (FULL, 3, 3, 1, 3, 0, 0), (FULL, 1, 1, 1, 1, 0, 0), (PROJECT, 0, 0, 0, 0, 0, 0),
        (FULL, 1, 1, 0, 1, 1, 0), (DIAG, 3, 3, 2, 3, 1, 0), (PROJECT, 1, 0, 0, 0, 0, 0), (PROJECT, 2, 0, 0, 0, 0, 0),
        (PROJECT, 3, 0, 0, 0, 0, 0),
    ],
    (2, 1): [
        (DIAG, 3, 3, 2, 3, 0, 0), (FULL, 2, 2, 1, 2, 0, 0), (FULL, 2, 2, 0, 2, 0, 0), (DIAG, 2, 2, 2, 2, 1, 0),
        (FULL, 1, 1, 0, 1, 0, 0), (DIAG, 1, 1, 2, 1, 0, 0), (FULL, 1, 1, 1, 1, 1, 0), (FULL, 3, 3, 0, 3, 0, 0),
        (FULL, 3, 3, 1, 3, 1, 0), (PROJECT, 0, 0, 0, 0, 0, 0), (PROJECT, 1, 0, 0, 0, 0, 0), (PROJECT, 2, 0, 0, 0, 0, 0),
        (PROJECT, 3, 0, 0, 0, 0, 0),
    ],
    (3, 0): [
        (FULL, 3, 3, 0, 3, 0, 0), (DIAG, 3, 3, 3, 3, 0, 0), (FULL, 2, 2, 2, 2, 0, 0), (FULL, 3, 3, 2, 3, 0, 0),
        (DIAG, 2, 2, 3, 2, 0, 0), (FULL, 2, 2, 0, 2, 0, 0), (FULL, 2, 2, 1, 2, 1, 0), (PROJECT, 0, 0, 0, 0, 0, 0),
        (PROJECT, 1, 0, 0, 0, 0, 0), (FULL, 3, 3, 1, 3, 1, 0), (PROJECT, 2, 0, 0, 0, 0, 0), (PROJECT, 3, 0, 0, 0, 0, 0),
    ],
    (3, 1): [
        (DIAG, 3, 3, 3, 3, 0, 0), (FULL, 1, 1, 2, 1, 0, 0), (FULL, 1, 1, 0, 1, 0, 0), (DIAG, 1, 1, 3, 1, 0, 0),
        (FULL, 3, 3, 0, 3, 0, 0), (FULL, 1, 1, 1, 1, 1, 0), (FULL, 2, 2, 1, 2, 0, 0), (FULL, 2, 2, 2, 2, 0, 0),
        (FULL, 2, 2, 0, 2, 0, 0), (DIAG, 2, 2, 3, 2, 1, 0), (PROJECT, 0, 0, 0, 0, 0, 0), (PROJECT, 1, 0, 0, 0, 0, 0),
        (FULL, 3, 3, 2, 3, 0, 0), (PROJECT, 2, 0, 0, 0, 0, 0), (FULL, 3, 3, 1, 3, 1, 0), (PROJECT, 3, 0, 0, 0, 0, 0),
    ],
}
N_TASKS = max(len(t) for t in TASKS.values())
KV_ORDER = {0: (1, 2, 0, 3), 1: (0, 1, 2, 3), 2: (2, 0, 1, 3), 3: (0, 3, 2, 1)}
OUT_ORDER = {0: (2, 3, 0, 1), 1: (1, 0, 2, 3), 2: (2, 3, 1, 0), 3: (2, 0, 1, 3)}

SENDS = {r: [(to, r[0], s, i) for s, tos in AFTER_KV[r].items() for to in tos for i in range(2)] for r in ROLES}
for _table in (PASS_Q, PASS_T):
    for _r, _steps in _table.items():
        SENDS[_r] += [m for messages in _steps.values() for m in messages]
_early = {r: {m[1:] for m in SENDS[r] if m[1] != r[0]} for r in ROLES}
for _r, _table in PASS_IN.items():
    SENDS[_r] += [(to, *m) for m, to in _table.items() if m not in _early[_r]]
N_SENDS = max(len(v) for v in SENDS.values())

PLACE = {r: {(r[0], s): s for s in range(SLOTS)} for r in ROLES}
for _p, _c in ROLES:
    for _to, _j, _s, _ in SENDS[_p, _c]:
        PLACE[_to, _c].setdefault((_j, _s), len(PLACE[_to, _c]))
N_KV = max(len(v) for v in PLACE.values())


def _task_waits(r):
    waits, seen = [], set(_early[r])
    for n, (kind, _, _, j, s, _, _) in enumerate(TASKS[r]):
        for i in range(2):
            if kind != PROJECT and j != r[0] and (j, s, i) not in seen:
                seen.add((j, s, i))
                waits.append((n, i, j, s, PASS_IN.get(r, {}).get((j, s, i))))
    return waits


def _query_waits(r):
    first = {}
    for n, (kind, at, *_) in enumerate(TASKS[r]):
        if kind != PROJECT and at >= SLOTS:
            first.setdefault(at, n)
    return [(n, at) for at, n in first.items()]


def _check():
    got = {r: set() for r in ROLES}
    for p, c in ROLES:
        for to, j, s, i in SENDS[p, c]:
            assert (j, s, i) not in got[to, c]
            got[to, c].add((j, s, i))
    for r in ROLES:
        need = {(j, s, i) for kind, _, _, j, s, _, _ in TASKS[r] if kind != PROJECT and j != r[0] for i in range(2)}
        assert got[r] == need | _early[r], r


_check()


def _pick(row, step, table):
    out = jnp.int32(0)
    for r, values in table.items():
        here = jnp.int32(0)
        for n, v in enumerate(values):
            if v:
                here = jnp.where(step == n, jnp.int32(v), here)
        out = jnp.where(row == r, here, out)
    return out


def _osend(s, h):
    n = SLOTS + 2 * s + h
    return n - SLOTS * (n // (SLOTS + 3))


def _dot(a, b, ca, cb):
    return lax.dot_general(a, b, (((ca,), (cb,)), ((), ())), preferred_element_type=jnp.float32)


def _kernel(x_ref, gain_ref, speed_ref, wq_ref, wk_ref, wv_ref, wo_ref, y_ref, a, w, q, kv, mix, top, ofin, osend, acc, cos, sin, gain_s,
            w_sem, wo_sem, x_sem, out_sem, a_send, a_recv, kv_send, kv_recv, q_send, q_recv, o_send, o_recv):
    own, depth = x_ref.shape
    tokens = 2 * own
    me = lax.axis_index("sp")
    chip, core = lax.div(me, CORES), lax.rem(me, CORES)
    other = CORES * chip + 1 - core
    e = HEAD**-0.5 * LOG2E
    group = CHIPS * CORES

    def half(h):
        return pl.ds(pl.multiple_of(h * own, own), own)

    def columns(n, width):
        return pl.ds(pl.multiple_of(n * width, width), width)

    def kv_weights(m):
        at, n = lax.rem(jnp.int32(m), 2), core * SLOTS + _pick(chip, m, KV_ORDER)
        return (pltpu.make_async_copy(wk_ref.at[:, columns(n, HEAD)], w.at[at, :, pl.ds(0, HEAD)], w_sem.at[at]),
                pltpu.make_async_copy(wv_ref.at[:, columns(n, HEAD)], w.at[at, :, pl.ds(HEAD, HEAD)], w_sem.at[at]))

    def query_weights(s):
        at, n = lax.rem(s, 2), core * SLOTS + s
        return pltpu.make_async_copy(wq_ref.at[:, columns(n, 2 * HEAD)], w.at[at], w_sem.at[at])

    def out_slot(n):
        return _pick(chip, n, OUT_ORDER)

    wide = 5 * HEAD
    n_wide = depth // wide

    def out_weights(n, k, t):
        head = jnp.where(k == 0, core, 1 - core) * SLOTS + out_slot(n)
        return pltpu.make_async_copy(wo_ref.at[columns(head, 2 * HEAD), columns(t, wide)], a.at[half(k), columns(t, wide)], wo_sem.at[k, t])

    pieces = 4
    piece = own // pieces

    def rows_in(n, c):
        return pl.ds(pl.multiple_of(c * own + n * piece, piece), piece)

    def load_x(n):
        return pltpu.make_async_copy(x_ref.at[pl.ds(n * piece, piece), :], a.at[rows_in(n, core)], x_sem.at[n])

    def send_a(n, c=None):
        rows = rows_in(n, core if c is None else c)
        return pltpu.make_async_remote_copy(
            src_ref=a.at[rows], dst_ref=a.at[rows], send_sem=a_send.at[n], recv_sem=a_recv.at[n],
            device_id={"sp": other}, device_id_type=MESH)

    for n in range(pieces):
        load_x(n).start()

    barrier = pltpu.get_barrier_semaphore()
    for n in range(1, group):
        pl.semaphore_signal(barrier, inc=1, device_id={"sp": lax.rem(me + n, group)}, device_id_type=MESH)

    def rows_of(i):
        return pl.ds(pl.multiple_of(lax.rem(core + i, 2) * tokens, tokens), tokens)

    def send(r, m):
        to, j, s, i = m
        at, n = PLACE[to, r[1]][j, s], SENDS[r].index(m)
        return pltpu.make_async_remote_copy(
            src_ref=kv.at[PLACE[r][j, s], rows_of(i)], dst_ref=kv.at[at, rows_of(i)], send_sem=kv_send.at[n],
            recv_sem=kv_recv.at[2 * (at - SLOTS) + i], device_id={"sp": CORES * to + r[1]}, device_id_type=MESH)

    def arrived(r, j, s, i):
        at = PLACE[r][j, s]
        pltpu.make_async_remote_copy(
            src_ref=kv.at[at, rows_of(i)], dst_ref=kv.at[at, rows_of(i)], send_sem=kv_send.at[0],
            recv_sem=kv_recv.at[2 * (at - SLOTS) + i], device_id={"sp": other}, device_id_type=MESH).wait_recv()

    def by_role(cases):
        for (p, c), actions in cases.items():
            if actions:
                @pl.when(me == CORES * p + c)
                def _(actions=actions):
                    for condition, action in actions:
                        pl.when(condition)(action)

    def pass_on(r, messages):
        for m in messages:
            if m[1] != r[0]:
                arrived(r, *m[1:])
            send(r, m).start()

    def pass_steps(table, step):
        return {r: [(step == n, functools.partial(pass_on, r, messages)) for n, messages in steps.items()] for r, steps in table.items()}

    def send_q(s, to):
        return pltpu.make_async_remote_copy(
            src_ref=q.at[s], dst_ref=q.at[SLOTS + s], send_sem=q_send.at[s], recv_sem=q_recv.at[s],
            device_id={"sp": CORES * to + core}, device_id_type=MESH)

    def send_o(source, head, to):
        return pltpu.make_async_remote_copy(
            src_ref=osend.at[source], dst_ref=ofin.at[:, columns(head, 2 * HEAD)], send_sem=o_send.at[source],
            recv_sem=o_recv.at[head], device_id={"sp": to}, device_id_type=MESH)

    def o_arrived(head):
        send_o(0, head, other).wait_recv()

    def table(i, _):
        n = 64
        here = pl.ds(pl.multiple_of(i * n, n), n)
        place = chip * tokens + i * n + lax.broadcasted_iota(jnp.int32, (n, HEAD // 2), 0)
        angle = place.astype(jnp.float32) * speed_ref[...]
        cos[here, :] = jnp.cos(angle)
        sin[here, :] = jnp.sin(angle)

    lax.fori_loop(0, own // 64, lambda i, _: table(core * (own // 64) + i, None), None)
    gain_s[...] = gain_ref[...].astype(jnp.float32)[None]
    for copy in kv_weights(0) + kv_weights(1):
        copy.start()
    pl.semaphore_wait(barrier, group - 1)
    rows, together = 32, 2

    for n in range(pieces):
        load_x(n).wait()

        def norm(i, _, n=n):
            for k in range(together):
                at = n * piece + (i * together + k) * rows
                here = pl.ds(pl.multiple_of(core * own + at, rows), rows)
                wide = a[here, :].astype(jnp.float32)
                acc[pl.ds(pl.multiple_of(at, rows), rows), :] = wide
                scale = lax.rsqrt(jnp.mean(wide * wide, -1, keepdims=True) + 1e-6)
                a[here, :] = (wide * scale * gain_s[...]).astype(a.dtype)

        lax.fori_loop(0, piece // (rows * together), norm, None)
        send_a(n).start()

    def turned(t, cos, sin):
        t = t.astype(jnp.bfloat16).astype(jnp.float32)
        u, v = t[:, : HEAD // 2], t[:, HEAD // 2 :]
        return jnp.concatenate([u * cos - v * sin, v * cos + u * sin], -1).astype(jnp.bfloat16)

    def kv_step(n, _):
        m = jnp.where(n < 4, lax.rem(n, 2), lax.div(n, 2))
        i = jnp.where(n < 4, lax.div(n, 2), lax.rem(n, 2))
        s, h, at = _pick(chip, m, KV_ORDER), lax.rem(core + i, 2), lax.rem(m, 2)

        @pl.when(i == 0)
        def _():
            for copy in kv_weights(m):
                copy.wait()

        @pl.when(n == 2)
        def _():
            lax.fori_loop(0, own // 64, lambda i, _: table((1 - core) * (own // 64) + i, None), None)
            for k in range(pieces):
                send_a(k, 1 - core).wait_recv()

        got = jnp.dot(a[half(h), :], w[at], preferred_element_type=jnp.float32)
        kv[s, pl.ds(pl.multiple_of(h * tokens, own), own), :] = turned(got[:, :HEAD], cos[half(h), :], sin[half(h), :])
        values = got[:, HEAD:].astype(jnp.bfloat16).T
        for b in range(own // HEAD):
            place = pl.ds(pl.multiple_of(h * tokens + own + b * HEAD, HEAD), HEAD)
            kv[s, place, :] = values[:, b * HEAD : (b + 1) * HEAD]

        @pl.when((i == 1) & (m < SLOTS - 2))
        def _():
            for copy in kv_weights(m + 2):
                copy.start()

        @pl.when((i == 1) & (m >= SLOTS - 2))
        def _():
            query_weights(m - (SLOTS - 2)).start()

        def go(r, s, half):
            for to in AFTER_KV[r][s]:
                send(r, (to, r[0], s, half)).start()

        by_role({r: [((s == c) & (i == k), functools.partial(go, r, c, k)) for c in steps for k in range(2)] for r, steps in AFTER_KV.items()})

    lax.fori_loop(0, 2 * SLOTS, kv_step, None)

    def q_step(s, _):
        at = lax.rem(s, 2)
        query_weights(s).wait()
        for h in range(2):
            for g in range(2):
                got = jnp.dot(a[half(h), :], w[at, :, g * HEAD : (g + 1) * HEAD], preferred_element_type=jnp.float32)
                q[s, pl.ds(g * tokens + h * own, own), :] = turned(got, cos[half(h), :], sin[half(h), :])

        @pl.when(s < SLOTS - 2)
        def _():
            query_weights(s + 2).start()

        by_role({(p, c): [(s == k, functools.partial(lambda k, p: send_q(k, HOST[p]).start(), k, p)) for k in lent[c]]
                 for p, lent in LENT.items() for c in range(CORES)})
        by_role(pass_steps(PASS_Q, s))

    lax.fori_loop(0, SLOTS, q_step, None)
    for n in range(pieces):
        send_a(n).wait_send()
    for t in range(n_wide):
        for k in range(2):
            out_weights(0, k, t).start()

    def start_anew(state):
        top[state] = jnp.full(top.shape[1:], NEG, jnp.float32)
        mix[state] = jnp.zeros(mix.shape[1:], jnp.float32)

    lax.fori_loop(0, SLOTS + 1, lambda i, _: start_anew(i), None)

    strip = own
    n_strips = 2 * tokens // strip
    ones = jnp.ones((8, strip), jnp.bfloat16)

    def block(qs, state, at, h, strips):
        keys = kv[at, pl.ds(pl.multiple_of(h * tokens, strip), strip), :]
        values = [kv[at, pl.ds(pl.multiple_of(h * tokens + own + b * HEAD, HEAD), HEAD), :] for b in range(strip // HEAD)]
        values = jnp.concatenate([jnp.concatenate(values, axis=1), ones], axis=0)
        spans = [pl.ds(n * strip, strip) for n, _ in strips]
        scores = [_dot(keys, q[qs, span, :], 1, 1) for span in spans]
        weights, keeps = [], []
        for (_, masked), span, s in zip(strips, spans, scores):
            if masked:
                seen = lax.broadcasted_iota(jnp.int32, s.shape, 1) >= lax.broadcasted_iota(jnp.int32, s.shape, 0)
                s = jnp.where(seen, s, HIDDEN)
            old = top[state, :, span]
            new = jnp.maximum(old, s.max(axis=0, keepdims=True))
            top[state, :, span] = new
            weights.append(jnp.exp2((s - new) * e).astype(jnp.bfloat16))
            keeps.append(jnp.exp2((old - new) * e))
        for span, p, keep in zip(spans, weights, keeps):
            mix[state, :, span] = mix[state, :, span] * keep + _dot(values, p, 1, 0)

    def finish(qs, state):
        lent = qs >= SLOTS
        to = CORES * jnp.where(chip == HOST[3], 3, 2)

        @pl.when(qs > SLOTS)
        def _():
            send_o(SLOTS - 1, core * SLOTS + SLOTS - 1, other).wait_send()

        def part(m, _):
            h = lax.rem(core + 1 + m, 2)
            local = (h == core) & jnp.logical_not(lent)
            source = jnp.where(lent, _osend(qs - SLOTS, h), qs)
            for g in range(2):
                span = pl.ds(pl.multiple_of(g * tokens + h * own, own), own)
                out = (mix[state, :HEAD, span] * (1 / mix[state, HEAD : HEAD + 1, span])).T.astype(jnp.bfloat16)

                @pl.when(local)
                def _():
                    ofin[:, pl.ds(pl.multiple_of((core * SLOTS + qs) * 2 * HEAD + g * HEAD, HEAD), HEAD)] = out

                @pl.when(jnp.logical_not(local))
                def _():
                    osend[source, :, g * HEAD : (g + 1) * HEAD] = out

            @pl.when(lent)
            def _():
                send_o(source, core * SLOTS + qs - SLOTS, to + h).start()

            @pl.when(jnp.logical_not(lent) & (h != core))
            def _():
                send_o(source, core * SLOTS + qs, other).start()

        lax.fori_loop(0, 2, part, None)

    def project(n):
        s = out_slot(n)
        away = jnp.bool_(False)
        for p, lent in LENT.items():
            for c in range(CORES):
                for k in lent[c]:
                    away |= (me == CORES * p + c) & (s == k)

        def head(c):
            return ofin[:, columns(c * SLOTS + s, 2 * HEAD)]

        def part(t):
            return pl.ds(pl.multiple_of(t * wide, wide), wide)

        @pl.when(n < SLOTS - 1)
        def _():
            o_arrived((1 - core) * SLOTS + s)

            @pl.when(away)
            def _():
                o_arrived(core * SLOTS + s)

            def add(t, _):
                for k in range(2):
                    out_weights(n, k, t).wait()
                left = jnp.concatenate([head(core), head(1 - core)], axis=1)
                acc[:, part(t)] += jnp.dot(left, a[:, part(t)], preferred_element_type=jnp.float32)
                for k in range(2):
                    out_weights(n + 1, k, t).start()

            lax.fori_loop(0, n_wide, add, None)

        @pl.when(n == SLOTS - 1)
        def _():
            one = jnp.where(away, 1, 0)
            cores = [jnp.where(k == 0, core, 1 - core) for k in (one, 1 - one)]

            @pl.when(away)
            def _():
                o_arrived((1 - core) * SLOTS + s)

            def first(t, _):
                out_weights(n, one, t).wait()
                acc[:, part(t)] += jnp.dot(head(cores[0]), a[half(one), part(t)], preferred_element_type=jnp.float32)

            lax.fori_loop(0, n_wide, first, None)
            o_arrived(cores[1] * SLOTS + s)

            def last(t, _):
                out_weights(n, 1 - one, t).wait()
                got = acc[:, part(t)] + jnp.dot(head(cores[1]), a[half(1 - one), part(t)], preferred_element_type=jnp.float32)
                for b in range(wide // HEAD):
                    m = t * (wide // HEAD) + b
                    at = pl.ds(pl.multiple_of(lax.rem(m, 4) * own, own), own)
                    q[lax.div(m, 4), at, :] = got[:, b * HEAD : (b + 1) * HEAD].astype(q.dtype)
                    pltpu.make_async_copy(q.at[lax.div(m, 4), at, :], y_ref.at[:, columns(m, HEAD)], out_sem.at[m]).start()

            lax.fori_loop(0, n_wide, last, None)

    columns_of = [{CORES * p + c: [f(p, c, t) for t in TASKS[p, c]] for p, c in ROLES} for f in (
        lambda p, c, t: t[0], lambda p, c, t: t[1], lambda p, c, t: t[2], lambda p, c, t: PLACE[p, c].get(t[3:5], 0),
        lambda p, c, t: t[5], lambda p, c, t: t[6])]

    def task(n, _):
        by_role(pass_steps(PASS_T, n))
        by_role({r: [(n == t, functools.partial(lambda k: send_q(k, 0).wait_recv(), at - SLOTS)) for t, at in _query_waits(r)] for r in ROLES})
        kind, qs, state, at, end, reset = (_pick(me, n, t) for t in columns_of)

        @pl.when(reset == 1)
        def _():
            start_anew(state)

        def take(r, j, s, i, to):
            arrived(r, j, s, i)
            if to is not None:
                send(r, (to, j, s, i)).start()

        def part(i, _):
            by_role({r: [((n == t) & (i == k), functools.partial(take, r, j, s, k, to)) for t, k, j, s, to in _task_waits(r)] for r in ROLES})

            @pl.when(kind == FULL)
            def _():
                block(qs, state, at, lax.rem(core + i, 2), [(m, False) for m in range(n_strips)])

        @pl.when((kind == FULL) | (kind == DIAG))
        def _():
            lax.fori_loop(0, 2, part, None)

        @pl.when(kind == DIAG)
        def _():
            block(qs, state, at, 0, [(0, True), (1, False), (2, True), (3, False)])
            block(qs, state, at, 1, [(1, True), (3, True)])

        @pl.when(end == 1)
        def _():
            finish(qs, state)

        @pl.when(kind == PROJECT)
        def _():
            @pl.when(qs == SLOTS - 1)
            def _():
                for (p, c) in ROLES:
                    if p in LENT:
                        @pl.when(me == CORES * p + c)
                        def _(p=p, c=c):
                            for k in LENT[p][c]:
                                send_q(k, HOST[p]).wait_send()

            project(qs)

    lax.fori_loop(0, N_TASKS, task, None)

    for p, c in ROLES:
        @pl.when(me == CORES * p + c)
        def _(p=p, c=c):
            for m in SENDS[p, c]:
                send((p, c), m).wait_send()
            for s in range(SLOTS):
                again = s == SLOTS - 1 and any(host == p and len(LENT[guest][c]) > 1 for guest, host in HOST.items())
                if (p not in LENT or s not in LENT[p][c]) and not again:
                    send_o(s, c * SLOTS + s, other).wait_send()
            for guest, host in HOST.items():
                if host == p:
                    for s in LENT[guest][c]:
                        for h in range(2):
                            send_o(_osend(s, h), c * SLOTS + s, CORES * guest + h).wait_send()

    for m in range(depth // HEAD):
        pltpu.make_async_copy(q.at[m // 4, pl.ds(m % 4 * own, own), :], y_ref.at[:, pl.ds(m * HEAD, HEAD)], out_sem.at[m]).wait()


def _hand_over(y_ref, out_ref, held, sems):
    pieces = held.shape[0]

    def copies(n):
        rows = pl.ds(n * held.shape[1], held.shape[1])
        return (pltpu.make_async_copy(y_ref.at[rows, :], held.at[n], sems.at[0, n]),
                pltpu.make_async_copy(held.at[n], out_ref.at[rows, :], sems.at[1, n]))

    for n in range(pieces):
        copies(n)[0].start()
    for n in range(pieces):
        copies(n)[0].wait()
        copies(n)[1].start()
    for n in range(pieces):
        copies(n)[1].wait()


def hand_over(y):
    own, depth = y.shape
    pieces = 4
    anywhere = pl.BlockSpec(memory_space=pl.ANY)
    return pl.pallas_call(
        _hand_over,
        out_shape=jax.ShapeDtypeStruct(y.shape, y.dtype),
        in_specs=[anywhere],
        out_specs=anywhere,
        scratch_shapes=[pltpu.VMEM((pieces, own // pieces, depth), y.dtype), pltpu.SemaphoreType.DMA((2, pieces))],
        cost_estimate=pl.CostEstimate(flops=0, bytes_accessed=4 * own * depth, transcendentals=0),
    )(y)


def layer(x, gain, wq, wk, wv, wo):
    own, depth = x.shape
    tokens = 2 * own
    low, f32 = jnp.bfloat16, jnp.float32
    anywhere, vmem = pl.BlockSpec(memory_space=pl.ANY), pl.BlockSpec(memory_space=pltpu.VMEM)
    dma = pltpu.SemaphoreType.DMA
    n = HEAD // 2
    speed = jnp.asarray(np.float32(THETA) ** (-np.arange(n, dtype=np.float32) / np.float32(n)))[None]
    y = pl.pallas_call(
        _kernel,
        out_shape=jax.ShapeDtypeStruct(x.shape, low),
        in_specs=[anywhere, vmem, vmem, anywhere, anywhere, anywhere, anywhere],
        out_specs=anywhere,
        scratch_shapes=[
            pltpu.VMEM((tokens, depth), low),
            pltpu.VMEM((2, depth, 2 * HEAD), low),
            pltpu.VMEM((SLOTS + 2, 2 * tokens, HEAD), low),
            pltpu.VMEM((N_KV, 2 * tokens, HEAD), low),
            pltpu.VMEM((SLOTS + 1, HEAD + 8, 2 * tokens), f32),
            pltpu.VMEM((SLOTS + 1, 1, 2 * tokens), f32),
            pltpu.VMEM((own, wq.shape[1]), low),
            pltpu.VMEM((SLOTS + 3, own, 2 * HEAD), low),
            pltpu.VMEM((own, depth), f32),
            pltpu.VMEM((tokens, n), f32),
            pltpu.VMEM((tokens, n), f32),
            pltpu.VMEM((1, depth), f32),
            dma((2,)), dma((2, 3)), dma((4,)), dma((depth // HEAD,)), dma((4,)), dma((4,)), dma((N_SENDS,)), dma((2 * (N_KV - SLOTS),)),
            dma((2,)), dma((2,)), dma((SLOTS + 3,)), dma((2 * SLOTS,)),
        ],
        compiler_params=pltpu.CompilerParams(collective_id=0, has_side_effects=True, vmem_limit_bytes=67043328),
        cost_estimate=pl.CostEstimate(flops=66 * 10**9, bytes_accessed=70 * 10**6, transcendentals=20 * 10**6),
    )(x, gain, speed, wq, wk, wv, wo)
    return hand_over(y)


def solution(mesh):
    tokens, whole = P(("dp", "sp"), None), P(None, None)
    return jax.shard_map(
        layer,
        mesh=mesh,
        in_specs=(tokens, P(None), whole, whole, whole, whole),
        out_specs=tokens,
        check_vma=False,
    )
```
